128 devices in a mesh: rep: 1, dp: 128 (over x, y, z, core).
Axes of the slice: x: 4, y: 4, z: 4, core: 2. Of those that a mesh axis runs over, the one named last changes fastest.
Arguments:
- x: bfloat16 [128, 1024, 1536], P(('rep', 'dp'))
- dy: bfloat16 [128, 1024, 1536], P(('rep', 'dp'))
- w_gate: bfloat16 [2, 1536, 3584], replicated
- w_up: bfloat16 [2, 1536, 3584], replicated
- w_down: bfloat16 [2, 3584, 1536], replicated
- m_w_gate: float32 [2, 1536, 3584], P(None, 'dp')
- m_w_up: float32 [2, 1536, 3584], P(None, 'dp')
- m_w_down: float32 [2, 3584, 1536], P(None, 'dp')
- v_w_gate: float32 [2, 1536, 3584], P(None, 'dp')
- v_w_up: float32 [2, 1536, 3584], P(None, 'dp')
- v_w_down: float32 [2, 3584, 1536], P(None, 'dp')
Outputs:
- output 1: bfloat16 [2, 1536, 3584], P('rep')
- output 2: bfloat16 [2, 1536, 3584], P('rep')
- output 3: bfloat16 [2, 3584, 1536], P('rep')
- output 4: float32 [2, 1536, 3584], P('rep', 'dp')
- output 5: float32 [2, 1536, 3584], P('rep', 'dp')
- output 6: float32 [2, 3584, 1536], P('rep', 'dp')
- output 7: float32 [2, 1536, 3584], P('rep', 'dp')
- output 8: float32 [2, 1536, 3584], P('rep', 'dp')
- output 9: float32 [2, 3584, 1536], P('rep', 'dp')
All inputs are finite; a program needn't handle non-finite values.
Results may differ from the reference program's by a relative error of at most 0.022.
Values are sent between devices in bfloat16 or wider.
A program may use at most 1.5 GiB of HBM per device.

```python
import jax
import jax.numpy as jnp
from jax import lax

SEQUENCES = 128
TOKENS = 1024
D = 1536
FF = 3584
LAYERS = 2
NAMES = ("w_gate", "w_up", "w_down")
SHAPES = {"w_gate": (LAYERS, D, FF), "w_up": (LAYERS, D, FF), "w_down": (LAYERS, FF, D)}


def bump(key, n, height):
    away = (jnp.arange(n, dtype=jnp.int32) - jax.random.randint(key, (), 0, n, jnp.int32)) % n
    return jnp.where(away < n // 8, height, 1.0)


def together(key, own, strength):
    shared = jax.random.normal(key, own.shape[1:], jnp.float32)
    return (own + strength * shared) * lax.rsqrt(1 + strength * strength)


def setup_inputs(seed: int = 0, part: int = 0) -> dict:
    kx, kdy, ka, kb, kz, kf, kh, kl, *keys = jax.random.split(jax.random.key(seed), 8 + 3 * len(NAMES))
    kx, kdy, ka, kb = (jax.random.fold_in(k, part) for k in (kx, kdy, ka, kb))
    kw, km, kv = (keys[i::3] for i in range(3))
    shape = (SEQUENCES, TOKENS, D)
    much_x, much_dy = jax.random.uniform(kz, (2,), jnp.float32, 0.0, 1.0)
    loud = 2.0 ** jax.random.uniform(jax.random.fold_in(kz, 1), (), jnp.float32, -1.0, 2.0)
    layers = 2.0 ** jax.random.uniform(kl, (LAYERS, 1, 1), jnp.float32, -1.0, 1.0)
    x = together(ka, jax.random.normal(kx, shape, jnp.float32), much_x) * bump(kf, D, 4.0)
    dy = together(kb, jax.random.normal(kdy, shape, jnp.float32), much_dy)
    drawn = {"x": x.astype(jnp.bfloat16), "dy": (loud * dy * (SEQUENCES * TOKENS) ** -0.5).astype(jnp.bfloat16)}
    for key, name in zip(kw, NAMES, strict=True):
        w = jax.random.normal(key, SHAPES[name], jnp.float32) * SHAPES[name][1] ** -0.5
        drawn[name] = (w * {"w_gate": 1.0, "w_up": bump(kh, FF, 4.0), "w_down": layers}[name]).astype(jnp.bfloat16)
    for key, name in zip(km, NAMES, strict=True):
        drawn[f"m_{name}"] = 0.1 * jax.random.normal(key, SHAPES[name], jnp.float32)
    for key, name in zip(kv, NAMES, strict=True):
        drawn[f"v_{name}"] = loud * loud * jax.random.uniform(key, SHAPES[name], jnp.float32, 0.05, 0.15)
    return drawn


def matmul(a, w):
    return jnp.dot(a, w, preferred_element_type=jnp.float32).astype(jnp.bfloat16)


def normed(h):
    wide = h.astype(jnp.float32)
    scale = lax.rsqrt(jnp.mean(wide**2, -1, keepdims=True) + 1e-6)
    return (wide * scale).astype(jnp.bfloat16)


def layer(h, w):
    a = normed(h)
    gate = jnp.dot(a, w["w_gate"], preferred_element_type=jnp.float32)
    up = jnp.dot(a, w["w_up"], preferred_element_type=jnp.float32)
    return h + matmul((jax.nn.silu(gate) * up).astype(jnp.bfloat16), w["w_down"])


def adamw(w, m, v, g):
    m = 0.9 * m + 0.1 * g
    v = 0.95 * v + 0.05 * g * g
    step = m * lax.rsqrt(v + 1e-8) + 0.1 * w
    return (w - 0.02 * step).astype(jnp.bfloat16), m, v


def stack(weights, h):
    return lax.scan(lambda h, w: (layer(h, w), None), h, weights)[0]


def reference(x, dy, w_gate, w_up, w_down, m_w_gate, m_w_up, m_w_down, v_w_gate, v_w_up, v_w_down):
    weights = dict(zip(NAMES, (w_gate, w_up, w_down), strict=True))

    def take(so_far, sequence):
        h, by_y = sequence
        _, back = jax.vjp(lambda w: stack(w, h), weights)
        return jax.tree.map(lambda total, term: total + term.astype(jnp.float32), so_far, back(by_y)[0]), None

    none_yet = {name: jnp.zeros(w.shape, jnp.float32) for name, w in weights.items()}
    by_weights, _ = lax.scan(take, none_yet, (x, dy))
    gradients = [by_weights[name].astype(jnp.bfloat16).astype(jnp.float32) for name in NAMES]
    new = [
        adamw(w.astype(jnp.float32), m, v, g)
        for w, m, v, g in zip((w_gate, w_up, w_down), (m_w_gate, m_w_up, m_w_down), (v_w_gate, v_w_up, v_w_down), gradients, strict=True)
    ]
    return tuple(one[which] for which in range(3) for one in new)
```

```python
import functools

import jax
import jax.numpy as jnp
import numpy as np
from jax import lax
from jax.experimental import pallas as pl
from jax.experimental.pallas import tpu as pltpu
from jax.sharding import Mesh
from jax.sharding import PartitionSpec as P

MESH = pl.DeviceIdType.MESH
RING = ("x", "y", "z")
ALL = ("x", "y", "z", "core")
N = 4
F32, BF16 = jnp.float32, jnp.bfloat16
LANES = 256


ORDERS = ((0, 1, 2), (1, 2, 0), (2, 0, 1))


def add_blocks(lead, out, *terms):
    def one(i, _):
        at = (i,) if len(lead) == 1 else (i // N, i % N)
        total = terms[0].at[at][...].astype(F32) if lead else None
        for t in terms[1:]:
            total = total + t.at[at][...].astype(F32)
        out.at[at][...] = total.astype(out.dtype)
        return 0

    if lead:
        lax.fori_loop(0, int(np.prod(lead)), one, 0)
    else:
        total = terms[0][...].astype(F32)
        for t in terms[1:]:
            total = total + t[...].astype(F32)
        out[...] = total.astype(out.dtype)


def scatter_kernel(*refs):
    grads, outs, scratch = refs[:3], refs[3:6], refs[6:]
    per = 8
    me = [lax.axis_index(a) for a in RING]
    right = [lax.rem(i + 1, N) for i in me]
    left = [lax.rem(i + N - 1, N) for i in me]
    across = [lax.rem(i + 2, N) for i in me]

    barrier = pltpu.get_barrier_semaphore()
    for axis in range(3):
        for to in (right[axis], left[axis]):
            pl.semaphore_signal(barrier, inc=1, device_id={RING[axis]: to}, device_id_type=MESH)

    colours = []
    for m in range(3):
        own, rx1, rx2, relay2, sum2, rx3, relay3, sum3 = scratch[m * per : (m + 1) * per]
        colours.append((own, (rx1, rx2, rx3), (None, relay2, relay3), (None, sum2, sum3)))
    local_sem, send_sem, recv_sem = scratch[3 * per :]

    def source(m, phase, index, half):
        own, _, _, sums = colours[m]
        a, b, _ = ORDERS[m]
        if phase == 0:
            width = grads[m].shape[-1] // 2
            at = [slice(None)] * 3
            at[a] = index
            return grads[m].at[(*at, slice(None), pl.ds(half * width, width))]
        if phase == 1:
            first = [axis for axis in range(3) if axis != a][0] == b
            return own.at[2 + half, index] if first else own.at[2 + half, :, index]
        return sums[1].at[half, index]

    loads = []
    for m in range(3):
        a = ORDERS[m][0]
        for k, (index, half) in enumerate(((right[a], 1), (left[a], 0), (me[a], 0), (me[a], 1))):
            copy = pltpu.make_async_copy(source(m, 0, index, half), colours[m][0].at[k], local_sem.at[m, k])
            copy.start()
            loads.append(copy)

    pl.semaphore_wait(barrier, 6)

    pending = []
    for phase in range(3):
        lead = ((N, N), (N,), ())[phase]

        def send(m, k, src, to):
            axis = ORDERS[m][phase]
            copy = pltpu.make_async_remote_copy(
                src_ref=src,
                dst_ref=colours[m][1][phase].at[k],
                send_sem=send_sem.at[m, phase, k],
                recv_sem=recv_sem.at[m, phase, k],
                device_id={RING[axis]: to},
                device_id_type=MESH,
            )
            copy.start()
            pending.append(copy)
            return copy

        flights = []
        for m in range(3):
            axis = ORDERS[m][phase]
            flights.append(
                [
                    send(m, 0, source(m, phase, across[axis], 1), right[axis]),
                    send(m, 1, source(m, phase, across[axis], 0), left[axis]),
                ]
            )
        for m in range(3):
            axis = ORDERS[m][phase]
            flights[m] += [
                send(m, 2, source(m, phase, right[axis], 0), right[axis]),
                send(m, 3, source(m, phase, left[axis], 1), left[axis]),
            ]
        if phase == 0:
            for copy in loads:
                copy.wait()
        for k in range(2):
            for m in range(3):
                axis = ORDERS[m][phase]
                own, rx, relays, _ = colours[m]
                flights[m][k].wait_recv()
                to = (right, left)[k][axis]
                if phase == 0:
                    passed = own.at[k]
                    add_blocks(lead, passed, passed, rx[phase].at[k])
                else:
                    passed = relays[phase].at[k]
                    add_blocks(lead, passed, source(m, phase, to, 1 - k), rx[phase].at[k])
                flights[m].append(send(m, 4 + k, passed, to))
        for half in range(2):
            for m in range(3):
                axis = ORDERS[m][phase]
                own, rx, _, sums = colours[m]
                direct, relayed = (2, 5) if half == 0 else (3, 4)
                flights[m][direct].wait_recv()
                flights[m][relayed].wait_recv()
                mine = own.at[2 + half] if phase == 0 else source(m, phase, me[axis], half)
                target = mine if phase == 0 else sums[phase].at[half]
                add_blocks(lead, target, mine, rx[phase].at[direct], rx[phase].at[relayed])
    for copy in pending:
        copy.wait_send()
    for m in range(3):
        width = outs[m].shape[-1] // 2
        for half in range(2):
            outs[m][:, half * width : (half + 1) * width] = colours[m][3][2][half].astype(outs[m].dtype)


def sum_over_chips(grads):
    scratch = []
    for g in grads:
        rows, half = g.shape[-2], g.shape[-1] // 2
        for lead in ((4, N, N), (6, N, N), (6, N), (2, N), (2, N), (6,), (2,), (2,)):
            scratch.append(pltpu.VMEM((*lead, rows, half), BF16))
    scratch += [
        pltpu.SemaphoreType.DMA((3, 4)),
        pltpu.SemaphoreType.DMA((3, 3, 6)),
        pltpu.SemaphoreType.DMA((3, 3, 6)),
    ]
    return pl.pallas_call(
        scatter_kernel,
        name="sum_over_chips",
        out_shape=[jax.ShapeDtypeStruct(g.shape[-2:], BF16) for g in grads],
        in_specs=[pl.BlockSpec(memory_space=pl.ANY)] * 3,
        out_specs=[pl.BlockSpec(memory_space=pltpu.VMEM)] * 3,
        scratch_shapes=scratch,
        compiler_params=pltpu.CompilerParams(collective_id=0, has_side_effects=True, vmem_limit_bytes=40 * 2**20),
        cost_estimate=pl.CostEstimate(flops=100_000_000, bytes_accessed=60_000_000, transcendentals=0),
    )(*grads)


def grad_kernel(core, a, a_other, d, d_other, out):
    dims = (((0,), (0,)), ((), ()))
    total = lax.dot_general(a[...], d[...], dims, preferred_element_type=F32)
    total = total + lax.dot_general(a_other[...], d_other[...], dims, preferred_element_type=F32)
    out[...] = total.astype(out.dtype)


def pair_gradient(core, a, a_other, d, d_other, bm, bn):
    tokens, m = a.shape
    n = d.shape[1] // 2
    left = pl.BlockSpec((tokens, bm), lambda i, j, core: (0, i))
    side = pl.BlockSpec((tokens, bn), lambda i, j, core: (0, core[0] * (n // bn) + j))
    return pl.pallas_call(
        grad_kernel,
        name="pair_gradient",
        out_shape=jax.ShapeDtypeStruct((m, n), BF16),
        grid_spec=pltpu.PrefetchScalarGridSpec(
            num_scalar_prefetch=1,
            grid=(m // bm, n // bn),
            in_specs=[left, left, side, side],
            out_specs=pl.BlockSpec((bm, bn), lambda i, j, core: (i, j)),
        ),
        cost_estimate=pl.CostEstimate(flops=4 * tokens * m * n, bytes_accessed=4 * tokens * (m + n) + 2 * m * n, transcendentals=0),
    )(core, a, a_other, d, d_other)


def place_kernel(width, *refs):
    blocks, out = refs[0], refs[-1]
    rows = out.shape[1]
    parts = width // 2 // LANES
    for core in range(2):
        for part in range(parts):
            at = (core * parts + part) * LANES
            out[0, :, at : at + LANES] = blocks[core, part * rows : (part + 1) * rows, :]


def place(gathered, which, layer, shape, so_far):
    _, total, width = shape
    rows = total // 64
    size = gathered.shape[1] // 3
    in_specs = [pl.BlockSpec((2, size, LANES), lambda p: (p, which, 0))]
    args = [gathered]
    if so_far is not None:
        in_specs.append(pl.BlockSpec(memory_space=pl.ANY))
        args.append(so_far)
    return pl.pallas_call(
        functools.partial(place_kernel, width),
        name="place",
        out_shape=jax.ShapeDtypeStruct(shape, BF16),
        grid=(64,),
        in_specs=in_specs,
        out_specs=pl.BlockSpec((1, rows, width), lambda p: (layer, p, 0)),
        input_output_aliases={} if so_far is None else {1: 0},
        cost_estimate=pl.CostEstimate(flops=10_000_000, bytes_accessed=4 * total * width, transcendentals=0),
    )(*args)


def swap(t):
    return lax.ppermute(t, "core", [(0, 1), (1, 0)])


def dot(a, b, over=(1, 0)):
    return lax.dot_general(a, b, (((over[0],), (over[1],)), ((), ())), preferred_element_type=F32)


def scale_of(h):
    wide = h.astype(F32)
    return lax.rsqrt(jnp.mean(wide**2, -1, keepdims=True) + 1e-6)


def adamw(w, m, v, g):
    m = 0.9 * m + 0.1 * g
    v = 0.95 * v + 0.05 * g * g
    step = m * lax.rsqrt(v + 1e-8) + 0.1 * w
    return (w - 0.02 * step).astype(BF16), m, v


def local_step(x, dy, wg, wu, wd, *moments):
    ms, vs = moments[:3], moments[3:]
    weights = (wg, wu, wd)
    core = lax.axis_index("core")
    chip = (lax.axis_index("x") * N + lax.axis_index("y")) * N + lax.axis_index("z")
    which = core.astype(jnp.int32)[None]
    layers = wg.shape[0]

    h, back = x[0], dy[0]
    kept = []
    for n in range(layers):
        a = (h.astype(F32) * scale_of(h)).astype(BF16)
        gate, up = dot(a, wg[n]), dot(a, wu[n])
        act = (jax.nn.silu(gate) * up).astype(BF16)
        kept.append((h, a, swap(a), gate, up, act, swap(act)))
        if n < layers - 1:
            h = h + dot(act, wd[n]).astype(BF16)

    new = [[None] * layers for _ in range(9)]
    placed = [None] * 3
    gathered = [None] * layers
    for n in reversed(range(layers)):
        h, a, a_other, gate, up, act, act_other = kept[n]
        back_other = swap(back)
        d_act = dot(back, wd[n], (1, 1)).astype(BF16).astype(F32)
        s = jax.nn.sigmoid(gate)
        d_up = (d_act * (gate * s)).astype(BF16)
        d_gate = (d_act * up * (s * (1 + gate * (1 - s)))).astype(BF16)
        d_up_other, d_gate_other = swap(d_up), swap(d_gate)
        by_down = pair_gradient(which, act, act_other, back, back_other, 512, 768)
        if n > 0:
            d_a = (dot(d_gate, wg[n], (1, 1)) + dot(d_up, wu[n], (1, 1))).astype(BF16).astype(F32)
            wide, scale = h.astype(F32), scale_of(h)
            inner = jnp.mean(d_a * wide, -1, keepdims=True)
            back = back + (scale * d_a - wide * (scale * scale * scale * inner)).astype(BF16)
        by_gate = pair_gradient(which, a, a_other, d_gate, d_gate_other, 512, 896)
        by_up = pair_gradient(which, a, a_other, d_up, d_up_other, 512, 896)
        sums = sum_over_chips([g.reshape(N, N, N, -1, g.shape[1]) for g in (by_gate, by_up, by_down)])

        blocks = []
        for k, total in enumerate(sums):
            other = swap(total)
            rows, half = total.shape[0] // 2, total.shape[1]
            halves = jnp.where(core == 0, jnp.stack([total, other]), jnp.stack([other, total]))
            mine = lax.dynamic_slice_in_dim(halves, core * rows, rows, 1)
            g = jnp.concatenate([mine[0], mine[1]], 1).astype(F32)
            at = (chip * 2 + core) * rows
            w = lax.dynamic_slice(weights[k], (n, at, 0), (1, rows, 2 * half))[0].astype(F32)
            w, m, v = adamw(w, ms[k][n], vs[k][n], g)
            new[3 + k][n], new[6 + k][n] = m, v
            keep = jnp.where(core == 0, w[:, :half], w[:, half:])
            give = jnp.where(core == 0, w[:, half:], w[:, :half])
            take = swap(give)
            both = jnp.where(core == 0, jnp.concatenate([keep, take], 0), jnp.concatenate([take, keep], 0))
            blocks += [both[:, i : i + LANES] for i in range(0, half, LANES)]
        gathered[n] = lax.all_gather(jnp.concatenate(blocks, 0), ALL, axis=0, tiled=False)

    for n in reversed(range(layers)):
        for k in range(3):
            placed[k] = place(gathered[n], k, n, weights[k].shape, placed[k])
    return (*placed, *(jnp.stack(new[i]) for i in range(3, 9)))


def solution(mesh):
    torus = Mesh(np.asarray(mesh.devices).reshape(N, N, N, 2), ALL)
    moments = P(None, ALL, None)
    return jax.shard_map(
        local_step,
        mesh=torus,
        in_specs=(P(ALL), P(ALL), P(), P(), P(), *([moments] * 6)),
        out_specs=(P(), P(), P(), *([moments] * 6)),
        check_vma=False,
    )
```

```python
import functools

import jax
import jax.numpy as jnp
import numpy as np
from jax import lax
from jax.experimental import pallas as pl
from jax.experimental.pallas import tpu as pltpu
from jax.sharding import Mesh
from jax.sharding import PartitionSpec as P

MESH = pl.DeviceIdType.MESH
RING = ("x", "y", "z")
ALL = ("x", "y", "z", "core")
N = 4
F32, BF16 = jnp.float32, jnp.bfloat16
LANES = 256


ORDERS = ((0, 1, 2), (1, 2, 0), (2, 0, 1))


def add_blocks(lead, out, *terms):
    def one(i, _):
        at = (i,) if len(lead) == 1 else (i // N, i % N)
        total = terms[0].at[at][...].astype(F32) if lead else None
        for t in terms[1:]:
            total = total + t.at[at][...].astype(F32)
        out.at[at][...] = total.astype(out.dtype)
        return 0

    if lead:
        lax.fori_loop(0, int(np.prod(lead)), one, 0)
    else:
        total = terms[0][...].astype(F32)
        for t in terms[1:]:
            total = total + t[...].astype(F32)
        out[...] = total.astype(out.dtype)


def scatter_kernel(*refs):
    grads, outs, scratch = refs[:3], refs[3:6], refs[6:]
    per = 8
    me = [lax.axis_index(a) for a in RING]
    right = [lax.rem(i + 1, N) for i in me]
    left = [lax.rem(i + N - 1, N) for i in me]
    across = [lax.rem(i + 2, N) for i in me]

    barrier = pltpu.get_barrier_semaphore()
    for axis in range(3):
        for to in (right[axis], left[axis]):
            pl.semaphore_signal(barrier, inc=1, device_id={RING[axis]: to}, device_id_type=MESH)

    colours = []
    for m in range(3):
        own, rx1, rx2, relay2, sum2, rx3, relay3, sum3 = scratch[m * per : (m + 1) * per]
        colours.append((own, (rx1, rx2, rx3), (None, relay2, relay3), (None, sum2, sum3)))
    local_sem, send_sem, recv_sem = scratch[3 * per :]

    def source(m, phase, index, half):
        own, _, _, sums = colours[m]
        a, b, _ = ORDERS[m]
        if phase == 0:
            width = grads[m].shape[-1] // 2
            at = [slice(None)] * 3
            at[a] = index
            return grads[m].at[(*at, slice(None), pl.ds(half * width, width))]
        if phase == 1:
            first = [axis for axis in range(3) if axis != a][0] == b
            return own.at[2 + half, index] if first else own.at[2 + half, :, index]
        return sums[1].at[half, index]

    loads = []
    for m in range(3):
        a = ORDERS[m][0]
        for k, (index, half) in enumerate(((right[a], 1), (left[a], 0), (me[a], 0), (me[a], 1))):
            copy = pltpu.make_async_copy(source(m, 0, index, half), colours[m][0].at[k], local_sem.at[m, k])
            copy.start()
            loads.append(copy)

    pl.semaphore_wait(barrier, 6)

    pending = []
    for phase in range(3):
        lead = ((N, N), (N,), ())[phase]

        def send(m, k, src, to):
            axis = ORDERS[m][phase]
            copy = pltpu.make_async_remote_copy(
                src_ref=src,
                dst_ref=colours[m][1][phase].at[k],
                send_sem=send_sem.at[m, phase, k],
                recv_sem=recv_sem.at[m, phase, k],
                device_id={RING[axis]: to},
                device_id_type=MESH,
            )
            copy.start()
            pending.append(copy)
            return copy

        flights = []
        for m in range(3):
            axis = ORDERS[m][phase]
            flights.append(
                [
                    send(m, 0, source(m, phase, across[axis], 1), right[axis]),
                    send(m, 1, source(m, phase, across[axis], 0), left[axis]),
                ]
            )
        for m in range(3):
            axis = ORDERS[m][phase]
            flights[m] += [
                send(m, 2, source(m, phase, right[axis], 0), right[axis]),
                send(m, 3, source(m, phase, left[axis], 1), left[axis]),
            ]
        if phase == 0:
            for copy in loads:
                copy.wait()
        for k in range(2):
            for m in range(3):
                axis = ORDERS[m][phase]
                own, rx, relays, _ = colours[m]
                flights[m][k].wait_recv()
                to = (right, left)[k][axis]
                if phase == 0:
                    passed = own.at[k]
                    add_blocks(lead, passed, passed, rx[phase].at[k])
                else:
                    passed = relays[phase].at[k]
                    add_blocks(lead, passed, source(m, phase, to, 1 - k), rx[phase].at[k])
                flights[m].append(send(m, 4 + k, passed, to))
        for half in range(2):
            for m in range(3):
                axis = ORDERS[m][phase]
                own, rx, _, sums = colours[m]
                direct, relayed = (2, 5) if half == 0 else (3, 4)
                flights[m][direct].wait_recv()
                flights[m][relayed].wait_recv()
                mine = own.at[2 + half] if phase == 0 else source(m, phase, me[axis], half)
                target = mine if phase == 0 else sums[phase].at[half]
                add_blocks(lead, target, mine, rx[phase].at[direct], rx[phase].at[relayed])
    for copy in pending:
        copy.wait_send()
    for m in range(3):
        width = outs[m].shape[-1] // 2
        for half in range(2):
            outs[m][:, half * width : (half + 1) * width] = colours[m][3][2][half].astype(outs[m].dtype)


def sum_over_chips(grads):
    scratch = []
    for g in grads:
        rows, half = g.shape[-2], g.shape[-1] // 2
        for lead in ((4, N, N), (6, N, N), (6, N), (2, N), (2, N), (6,), (2,), (2,)):
            scratch.append(pltpu.VMEM((*lead, rows, half), BF16))
    scratch += [
        pltpu.SemaphoreType.DMA((3, 4)),
        pltpu.SemaphoreType.DMA((3, 3, 6)),
        pltpu.SemaphoreType.DMA((3, 3, 6)),
    ]
    return pl.pallas_call(
        scatter_kernel,
        name="sum_over_chips",
        out_shape=[jax.ShapeDtypeStruct(g.shape[-2:], BF16) for g in grads],
        in_specs=[pl.BlockSpec(memory_space=pl.ANY)] * 3,
        out_specs=[pl.BlockSpec(memory_space=pltpu.VMEM)] * 3,
        scratch_shapes=scratch,
        compiler_params=pltpu.CompilerParams(collective_id=0, has_side_effects=True, vmem_limit_bytes=40 * 2**20),
        cost_estimate=pl.CostEstimate(flops=40_000_000_000, bytes_accessed=60_000_000, transcendentals=0),
    )(*grads)


def grad_kernel(core, a, a_other, d, d_other, out):
    left, side = jnp.concatenate([a[...], a_other[...]], 0), jnp.concatenate([d[...], d_other[...]], 0)
    out[...] = lax.dot_general(left, side, (((0,), (0,)), ((), ())), preferred_element_type=F32).astype(out.dtype)


def pair_gradient(core, a, a_other, d, d_other, bm):
    tokens, m = a.shape
    n = d.shape[1] // 2
    left = pl.BlockSpec((tokens, bm), lambda i, core: (0, i))
    side = pl.BlockSpec((tokens, n), lambda i, core: (0, core[0]))
    return pl.pallas_call(
        grad_kernel,
        name="pair_gradient",
        out_shape=jax.ShapeDtypeStruct((m, n), BF16),
        grid_spec=pltpu.PrefetchScalarGridSpec(
            num_scalar_prefetch=1,
            grid=(m // bm,),
            in_specs=[left, left, side, side],
            out_specs=pl.BlockSpec((bm, n), lambda i, core: (i, 0)),
        ),
        compiler_params=pltpu.CompilerParams(vmem_limit_bytes=48 * 2**20),
        cost_estimate=pl.CostEstimate(flops=4 * tokens * m * n, bytes_accessed=4 * tokens * (m + n) + 2 * m * n, transcendentals=0),
    )(core, a, a_other, d, d_other)


def dot(a, b, over=(1, 0)):
    return lax.dot_general(a, b, (((over[0],), (over[1],)), ((), ())), preferred_element_type=F32)


def local_call(body, name, flops, moved, **kw):
    return pl.pallas_call(
        body,
        name=name,
        compiler_params=pltpu.CompilerParams(vmem_limit_bytes=60 * 2**20),
        cost_estimate=pl.CostEstimate(flops=flops, bytes_accessed=moved, transcendentals=0),
        **kw,
    )


def gated_kernel(a, w_gate, w_up, gate, up, act):
    g, u = dot(a[...], w_gate[...]), dot(a[...], w_up[...])
    gate[...] = g
    up[...] = u
    act[...] = (g * jax.nn.sigmoid(g) * u).astype(act.dtype)


def gated(a, w_gate, w_up, layer, bn=512):
    tokens, d = a.shape
    ff = w_gate.shape[2]
    weight = pl.BlockSpec((None, d, bn), lambda j: (layer, 0, j))
    out = pl.BlockSpec((tokens, bn), lambda j: (0, j))
    return local_call(
        gated_kernel,
        "gated",
        4 * tokens * d * ff,
        4 * d * ff + 10 * tokens * ff,
        out_shape=[jax.ShapeDtypeStruct((tokens, ff), t) for t in (F32, F32, BF16)],
        grid=(ff // bn,),
        in_specs=[pl.BlockSpec((tokens, d), lambda j: (0, 0)), weight, weight],
        out_specs=[out] * 3,
    )(a, w_gate, w_up)


def gated_back_kernel(back, w_down, gate, up, d_gate, d_up):
    d_act = dot(back[...], w_down[...], (1, 1)).astype(BF16).astype(F32)
    g, u = gate[...], up[...]
    s = jax.nn.sigmoid(g)
    d_up[...] = (d_act * (g * s)).astype(d_up.dtype)
    d_gate[...] = (d_act * u * (s * (1 + g * (1 - s)))).astype(d_gate.dtype)


def gated_back(back, w_down, gate, up, layer, bn=512):
    tokens, d = back.shape
    ff = gate.shape[1]
    wide = pl.BlockSpec((tokens, bn), lambda j: (0, j))
    return local_call(
        gated_back_kernel,
        "gated_back",
        2 * tokens * d * ff,
        2 * d * ff + 12 * tokens * ff,
        out_shape=[jax.ShapeDtypeStruct((tokens, ff), BF16)] * 2,
        grid=(ff // bn,),
        in_specs=[pl.BlockSpec((tokens, d), lambda j: (0, 0)), pl.BlockSpec((None, bn, d), lambda j: (layer, j, 0)), wide, wide],
        out_specs=[wide] * 2,
    )(back, w_down, gate, up)


def normed_back_kernel(d_gate, d_up, w_gate, w_up, h, back, out):
    d_a = dot(d_gate[...], w_gate[...], (1, 1)) + dot(d_up[...], w_up[...], (1, 1))
    d_a, wide = d_a.astype(BF16).astype(F32), h[...].astype(F32)
    scale = lax.rsqrt(jnp.mean(wide**2, -1, keepdims=True) + 1e-6)
    inner = jnp.mean(d_a * wide, -1, keepdims=True)
    out[...] = back[...] + (scale * d_a - wide * (scale * scale * scale * inner)).astype(BF16)


def normed_back(d_gate, d_up, w_gate, w_up, h, back, layer, bt=256):
    tokens, d = h.shape
    ff = d_gate.shape[1]
    wide = pl.BlockSpec((bt, ff), lambda i: (i, 0))
    weight = pl.BlockSpec((None, d, ff), lambda i: (layer, 0, 0), pipeline_mode=pl.Buffered(1))
    narrow = pl.BlockSpec((bt, d), lambda i: (i, 0))
    return local_call(
        normed_back_kernel,
        "normed_back",
        4 * tokens * d * ff,
        4 * d * ff + 4 * tokens * ff,
        out_shape=jax.ShapeDtypeStruct((tokens, d), BF16),
        grid=(tokens // bt,),
        in_specs=[wide, wide, weight, weight, narrow, narrow],
        out_specs=narrow,
    )(d_gate, d_up, w_gate, w_up, h, back)


def place_kernel(rows, *refs):
    blocks, out = refs[0], refs[-1]
    parts = out.shape[2] // 2 // LANES

    def one(chip, _):
        for core in range(2):
            for part in range(parts):
                at = (core * parts + part) * LANES
                out[0, pl.ds(chip * rows, rows), at : at + LANES] = blocks[chip * 2 + core, part * rows : (part + 1) * rows, :]
        return 0

    lax.fori_loop(0, out.shape[1] // rows, one, 0)


def place(gathered, which, layer, shape, so_far, steps=8):
    _, total, width = shape
    rows = total // 64
    chips = 64 // steps
    size = gathered.shape[1] // 3
    in_specs = [pl.BlockSpec((2 * chips, size, LANES), lambda p: (p, which, 0))]
    args = [gathered]
    if so_far is not None:
        in_specs.append(pl.BlockSpec(memory_space=pl.ANY))
        args.append(so_far)
    return local_call(
        functools.partial(place_kernel, rows),
        "place",
        100_000_000,
        4 * total * width,
        out_shape=jax.ShapeDtypeStruct(shape, BF16),
        grid=(steps,),
        in_specs=in_specs,
        out_specs=pl.BlockSpec((1, rows * chips, width), lambda p: (layer, p, 0)),
        input_output_aliases={} if so_far is None else {1: 0},
    )(*args)


def tied(*ts):
    return lax.optimization_barrier(ts)


def gather(blocks):
    return lax.all_gather(blocks, ALL, axis=0, tiled=False)


def swap(t):
    return lax.ppermute(t, "core", [(0, 1), (1, 0)])


def scale_of(h):
    wide = h.astype(F32)
    return lax.rsqrt(jnp.mean(wide**2, -1, keepdims=True) + 1e-6)


def adamw(w, m, v, g):
    m = 0.9 * m + 0.1 * g
    v = 0.95 * v + 0.05 * g * g
    step = m * lax.rsqrt(v + 1e-8) + 0.1 * w
    return (w - 0.02 * step).astype(BF16), m, v


def local_step(x, dy, wg, wu, wd, *moments):
    ms, vs = moments[:3], moments[3:]
    weights = (wg, wu, wd)
    core = lax.axis_index("core")
    chip = (lax.axis_index("x") * N + lax.axis_index("y")) * N + lax.axis_index("z")
    which = core.astype(jnp.int32)[None]
    layers = wg.shape[0]

    h, back = x[0], dy[0]
    kept = []
    last = layers - 1
    back_other = swap(back)
    for n in range(layers):
        a = (h.astype(F32) * scale_of(h)).astype(BF16)
        a_other = swap(a)
        gate, up, act = gated(a, wg, wu, n)
        if n > 0:
            act, back_other, kept[n - 1][2], kept[n - 1][6] = tied(act, back_other, kept[n - 1][2], kept[n - 1][6])
        kept.append([h, a, a_other, gate, up, act, swap(act)])
        if n < last:
            h = h + dot(act, wd[n]).astype(BF16)

    new = [[None] * layers for _ in range(9)]
    placed = [None] * 3
    gathered = [None] * layers
    pending = None
    for n in reversed(range(layers)):
        h, a, a_other, gate, up, act, act_other = kept[n]
        if n < last:
            back_other = swap(back)
        d_gate, d_up = gated_back(back, wd, gate, up, n)
        d_up_other, d_gate_other = swap(d_up), swap(d_gate)
        if pending is not None:
            d_gate, d_up, pending = tied(d_gate, d_up, pending)
            gathered[n + 1] = gather(pending)
        if n > 0:
            below = normed_back(d_gate, d_up, wg, wu, h, back, n)
            d_gate, d_up, below = tied(d_gate, d_up, below)
        by_down = pair_gradient(which, act, act_other, back, back_other, 896)
        by_gate = pair_gradient(which, a, a_other, d_gate, d_gate_other, 512)
        by_up = pair_gradient(which, a, a_other, d_up, d_up_other, 512)
        sums = sum_over_chips([g.reshape(N, N, N, -1, g.shape[1]) for g in (by_gate, by_up, by_down)])
        if n > 0:
            back, *sums = tied(below, *sums)

        blocks = []
        for k, total in enumerate(sums):
            other = swap(total)
            rows, half = total.shape[0] // 2, total.shape[1]
            halves = jnp.where(core == 0, jnp.stack([total, other]), jnp.stack([other, total]))
            mine = lax.dynamic_slice_in_dim(halves, core * rows, rows, 1)
            g = jnp.concatenate([mine[0], mine[1]], 1).astype(F32)
            at = (chip * 2 + core) * rows
            w = lax.dynamic_slice(weights[k], (n, at, 0), (1, rows, 2 * half))[0].astype(F32)
            w, m, v = adamw(w, ms[k][n], vs[k][n], g)
            new[3 + k][n], new[6 + k][n] = m, v
            keep = jnp.where(core == 0, w[:, :half], w[:, half:])
            give = jnp.where(core == 0, w[:, half:], w[:, :half])
            take = swap(give)
            both = jnp.where(core == 0, jnp.concatenate([keep, take], 0), jnp.concatenate([take, keep], 0))
            blocks += [both[:, i : i + LANES] for i in range(0, half, LANES)]
        pending = jnp.concatenate(blocks, 0)
        if n == 0:
            pending, *gathered[1:] = tied(pending, *gathered[1:])
            gathered[0] = gather(pending)

    for n in reversed(range(layers)):
        for k in range(3):
            placed[k] = place(gathered[n], k, n, weights[k].shape, placed[k])
    return (*placed, *(jnp.stack(new[i]) for i in range(3, 9)))


def solution(mesh):
    torus = Mesh(np.asarray(mesh.devices).reshape(N, N, N, 2), ALL)
    moments = P(None, ALL, None)
    return jax.shard_map(
        local_step,
        mesh=torus,
        in_specs=(P(ALL), P(ALL), P(), P(), P(), *([moments] * 6)),
        out_specs=(P(), P(), P(), *([moments] * 6)),
        check_vma=False,
    )
```

```python
import functools

import jax
import jax.numpy as jnp
import numpy as np
from jax import lax
from jax.experimental import pallas as pl
from jax.experimental.pallas import tpu as pltpu
from jax.sharding import Mesh
from jax.sharding import PartitionSpec as P

MESH = pl.DeviceIdType.MESH
RING = ("x", "y", "z")
ALL = ("x", "y", "z", "core")
N = 4
F32, BF16 = jnp.float32, jnp.bfloat16
LANES = 256


ORDERS = ((0, 1, 2), (1, 2, 0), (2, 0, 1))


def add_blocks(lead, out, *terms):
    def one(i, _):
        at = (i,) if len(lead) == 1 else (i // N, i % N)
        total = terms[0].at[at][...].astype(F32) if lead else None
        for t in terms[1:]:
            total = total + t.at[at][...].astype(F32)
        out.at[at][...] = total.astype(out.dtype)
        return 0

    if lead:
        lax.fori_loop(0, int(np.prod(lead)), one, 0)
    else:
        total = terms[0][...].astype(F32)
        for t in terms[1:]:
            total = total + t[...].astype(F32)
        out[...] = total.astype(out.dtype)


def scatter_kernel(work, *refs):
    ins, made = (work.inputs, work.outputs) if work else (0, 0)
    grads, given, refs = refs[:3], refs[3 : 3 + ins], refs[3 + ins :]
    outs, making, scratch = refs[:3], refs[3 : 3 + made], refs[3 + made :]
    per = 8
    me = [lax.axis_index(a) for a in RING]
    right = [lax.rem(i + 1, N) for i in me]
    left = [lax.rem(i + N - 1, N) for i in me]
    across = [lax.rem(i + 2, N) for i in me]

    barrier = pltpu.get_barrier_semaphore()
    for axis in range(3):
        for to in (right[axis], left[axis]):
            pl.semaphore_signal(barrier, inc=1, device_id={RING[axis]: to}, device_id_type=MESH)
    if work:
        pl.semaphore_signal(barrier, inc=1, device_id={"core": 1 - lax.axis_index("core")}, device_id_type=MESH)

    colours = []
    for m in range(3):
        own, rx1, rx2, relay2, sum2, rx3, relay3, sum3 = scratch[m * per : (m + 1) * per]
        colours.append((own, (rx1, rx2, rx3), (None, relay2, relay3), (None, sum2, sum3)))
    local_sem, send_sem, recv_sem, *work_sem = scratch[3 * per :]

    def source(m, phase, index, half):
        own, _, _, sums = colours[m]
        a, b, _ = ORDERS[m]
        if phase == 0:
            width = grads[m].shape[-1] // 2
            at = [slice(None)] * 3
            at[a] = index
            return grads[m].at[(*at, slice(None), pl.ds(half * width, width))]
        if phase == 1:
            first = [axis for axis in range(3) if axis != a][0] == b
            return own.at[2 + half, index] if first else own.at[2 + half, :, index]
        return sums[1].at[half, index]

    loads = []
    for m in range(3):
        a = ORDERS[m][0]
        for k, (index, half) in enumerate(((right[a], 1), (left[a], 0), (me[a], 0), (me[a], 1))):
            copy = pltpu.make_async_copy(source(m, 0, index, half), colours[m][0].at[k], local_sem.at[m, k])
            copy.start()
            loads.append(copy)

    pl.semaphore_wait(barrier, 7 if work else 6)

    pending = []
    for phase in range(3):
        lead = ((N, N), (N,), ())[phase]

        def send(m, k, src, to):
            axis = ORDERS[m][phase]
            copy = pltpu.make_async_remote_copy(
                src_ref=src,
                dst_ref=colours[m][1][phase].at[k],
                send_sem=send_sem.at[m, phase, k],
                recv_sem=recv_sem.at[m, phase, k],
                device_id={RING[axis]: to},
                device_id_type=MESH,
            )
            copy.start()
            pending.append(copy)
            return copy

        flights = []
        for m in range(3):
            axis = ORDERS[m][phase]
            flights.append(
                [
                    send(m, 0, source(m, phase, across[axis], 1), right[axis]),
                    send(m, 1, source(m, phase, across[axis], 0), left[axis]),
                ]
            )
        for m in range(3):
            axis = ORDERS[m][phase]
            flights[m] += [
                send(m, 2, source(m, phase, right[axis], 0), right[axis]),
                send(m, 3, source(m, phase, left[axis], 1), left[axis]),
            ]
        if phase == 0:
            for copy in loads:
                copy.wait()
            if work:
                work.first(given, making)
        for k in range(2):
            for m in range(3):
                axis = ORDERS[m][phase]
                own, rx, relays, _ = colours[m]
                flights[m][k].wait_recv()
                to = (right, left)[k][axis]
                if phase == 0:
                    passed = own.at[k]
                    add_blocks(lead, passed, passed, rx[phase].at[k])
                else:
                    passed = relays[phase].at[k]
                    add_blocks(lead, passed, source(m, phase, to, 1 - k), rx[phase].at[k])
                flights[m].append(send(m, 4 + k, passed, to))
        if phase == 0 and work:
            handed = work.second(given, making, *work_sem)
        for half in range(2):
            for m in range(3):
                axis = ORDERS[m][phase]
                own, rx, _, sums = colours[m]
                direct, relayed = (2, 5) if half == 0 else (3, 4)
                flights[m][direct].wait_recv()
                flights[m][relayed].wait_recv()
                mine = own.at[2 + half] if phase == 0 else source(m, phase, me[axis], half)
                target = mine if phase == 0 else sums[phase].at[half]
                add_blocks(lead, target, mine, rx[phase].at[direct], rx[phase].at[relayed])
    for copy in pending:
        copy.wait_send()
    if work:
        for copy in handed:
            copy.wait()
    for m in range(3):
        width = outs[m].shape[-1] // 2
        for half in range(2):
            outs[m][:, half * width : (half + 1) * width] = colours[m][3][2][half].astype(outs[m].dtype)


def sum_over_chips(grads, work=None, given=()):
    scratch = []
    for g in grads:
        rows, half = g.shape[-2], g.shape[-1] // 2
        for lead in ((4, N, N), (6, N, N), (6, N), (2, N), (2, N), (6,), (2,), (2,)):
            scratch.append(pltpu.VMEM((*lead, rows, half), BF16))
    scratch += [
        pltpu.SemaphoreType.DMA((3, 4)),
        pltpu.SemaphoreType.DMA((3, 3, 6)),
        pltpu.SemaphoreType.DMA((3, 3, 6)),
    ]
    anywhere = pl.BlockSpec(memory_space=pl.ANY)
    out_shape = [jax.ShapeDtypeStruct(g.shape[-2:], BF16) for g in grads]
    out_specs = [pl.BlockSpec(memory_space=pltpu.VMEM)] * 3
    if work:
        scratch += [pltpu.SemaphoreType.DMA((2,)), pltpu.SemaphoreType.DMA((2,))]
        out_shape += work.shapes
        out_specs += [anywhere] * work.outputs
    return pl.pallas_call(
        functools.partial(scatter_kernel, work),
        name="sum_over_chips",
        out_shape=out_shape,
        in_specs=[anywhere] * (3 + len(given)),
        out_specs=out_specs,
        scratch_shapes=scratch,
        compiler_params=pltpu.CompilerParams(collective_id=1 if work else 0, has_side_effects=True, vmem_limit_bytes=60 * 2**20),
        cost_estimate=pl.CostEstimate(flops=40_000_000_000, bytes_accessed=60_000_000, transcendentals=0),
    )(*grads, *given)


class LayerBelow:
    inputs, outputs = 7, 7

    def __init__(self, tokens, d, ff):
        self.tokens, self.d, self.ff = tokens, d, ff
        half = jax.ShapeDtypeStruct((tokens, ff // 2), BF16)
        self.shapes = [jax.ShapeDtypeStruct((ff, d // 2), BF16)] + [half] * 6

    def first(self, given, making, bm=512):
        act, act_other, back, back_other = given[:4]
        tokens, half = self.tokens, self.d // 2
        core = lax.axis_index("core")

        def step(act, act_other, back, back_other, out):
            dims = (((0,), (0,)), ((), ()))
            total = lax.dot_general(act[...], back[...], dims, preferred_element_type=F32)
            total = total + lax.dot_general(act_other[...], back_other[...], dims, preferred_element_type=F32)
            out[...] = total.astype(out.dtype)

        left = pl.BlockSpec((tokens, bm), lambda i: (0, i))
        side = pl.BlockSpec((tokens, half), lambda i: (0, core))
        pltpu.emit_pipeline(
            step,
            grid=(self.ff // bm,),
            in_specs=[left, left, side, side],
            out_specs=[pl.BlockSpec((bm, half), lambda i: (i, 0))],
        )(act, act_other, back, back_other, making[0])

    def second(self, given, making, send_sem, recv_sem, bn=256):
        back, w_down, gate, up = given[2], given[4], given[5], given[6]
        mine, theirs, others = making[1:3], making[3:5], making[5:7]
        core = lax.axis_index("core")
        blocks = self.ff // 2 // bn
        copies = []
        for half, outs in ((1 - core, theirs), (core, mine)):
            first = half * blocks
            wide = pl.BlockSpec((self.tokens, bn), lambda j, first=first: (0, first + j))
            out = pl.BlockSpec((self.tokens, bn), lambda j: (0, j))
            pltpu.emit_pipeline(
                gated_back_kernel,
                grid=(blocks,),
                in_specs=[
                    pl.BlockSpec((self.tokens, self.d), lambda j: (0, 0)),
                    pl.BlockSpec((bn, self.d), lambda j, first=first: (first + j, 0)),
                    wide,
                    wide,
                ],
                out_specs=[out, out],
            )(back, w_down.at[0], gate, up, *outs)
            if outs is theirs:
                for k in range(2):
                    copy = pltpu.make_async_remote_copy(
                        src_ref=theirs[k],
                        dst_ref=others[k],
                        send_sem=send_sem.at[k],
                        recv_sem=recv_sem.at[k],
                        device_id={"core": 1 - core},
                        device_id_type=MESH,
                    )
                    copy.start()
                    copies.append(copy)
        return copies


def grad_kernel(core, a, a_other, d, d_other, out):
    left, side = jnp.concatenate([a[...], a_other[...]], 0), jnp.concatenate([d[...], d_other[...]], 0)
    out[...] = lax.dot_general(left, side, (((0,), (0,)), ((), ())), preferred_element_type=F32).astype(out.dtype)


def pair_gradient(core, a, a_other, d, d_other, bm, halved=False):
    tokens, m = a.shape
    n = d.shape[1] if halved else d.shape[1] // 2
    left = pl.BlockSpec((tokens, bm), lambda i, core: (0, i))
    side = pl.BlockSpec((tokens, n), lambda i, core: (0, 0 if halved else core[0]))
    return pl.pallas_call(
        grad_kernel,
        name="pair_gradient",
        out_shape=jax.ShapeDtypeStruct((m, n), BF16),
        grid_spec=pltpu.PrefetchScalarGridSpec(
            num_scalar_prefetch=1,
            grid=(m // bm,),
            in_specs=[left, left, side, side],
            out_specs=pl.BlockSpec((bm, n), lambda i, core: (i, 0)),
        ),
        compiler_params=pltpu.CompilerParams(vmem_limit_bytes=48 * 2**20),
        cost_estimate=pl.CostEstimate(flops=4 * tokens * m * n, bytes_accessed=4 * tokens * (m + n) + 2 * m * n, transcendentals=0),
    )(core, a, a_other, d, d_other)


def dot(a, b, over=(1, 0)):
    return lax.dot_general(a, b, (((over[0],), (over[1],)), ((), ())), preferred_element_type=F32)


def local_call(body, name, flops, moved, **kw):
    return pl.pallas_call(
        body,
        name=name,
        compiler_params=pltpu.CompilerParams(vmem_limit_bytes=60 * 2**20),
        cost_estimate=pl.CostEstimate(flops=flops, bytes_accessed=moved, transcendentals=0),
        **kw,
    )


def gated_kernel(a, w_gate, w_up, gate, up, act):
    g, u = dot(a[...], w_gate[...]), dot(a[...], w_up[...])
    gate[...] = g
    up[...] = u
    act[...] = (g * jax.nn.sigmoid(g) * u).astype(act.dtype)


def gated(a, w_gate, w_up, layer, bn=512):
    tokens, d = a.shape
    ff = w_gate.shape[2]
    weight = pl.BlockSpec((None, d, bn), lambda j: (layer, 0, j))
    out = pl.BlockSpec((tokens, bn), lambda j: (0, j))
    return local_call(
        gated_kernel,
        "gated",
        4 * tokens * d * ff,
        4 * d * ff + 10 * tokens * ff,
        out_shape=[jax.ShapeDtypeStruct((tokens, ff), t) for t in (F32, F32, BF16)],
        grid=(ff // bn,),
        in_specs=[pl.BlockSpec((tokens, d), lambda j: (0, 0)), weight, weight],
        out_specs=[out] * 3,
    )(a, w_gate, w_up)


def gated_back_kernel(back, w_down, gate, up, d_gate, d_up):
    d_act = dot(back[...], w_down[...], (1, 1)).astype(BF16).astype(F32)
    g, u = gate[...], up[...]
    s = jax.nn.sigmoid(g)
    d_up[...] = (d_act * (g * s)).astype(d_up.dtype)
    d_gate[...] = (d_act * u * (s * (1 + g * (1 - s)))).astype(d_gate.dtype)


def gated_back(back, w_down, gate, up, layer, bn=512):
    tokens, d = back.shape
    ff = gate.shape[1]
    wide = pl.BlockSpec((tokens, bn), lambda j: (0, j))
    return local_call(
        gated_back_kernel,
        "gated_back",
        2 * tokens * d * ff,
        2 * d * ff + 12 * tokens * ff,
        out_shape=[jax.ShapeDtypeStruct((tokens, ff), BF16)] * 2,
        grid=(ff // bn,),
        in_specs=[pl.BlockSpec((tokens, d), lambda j: (0, 0)), pl.BlockSpec((None, bn, d), lambda j: (layer, j, 0)), wide, wide],
        out_specs=[wide] * 2,
    )(back, w_down, gate, up)


def normed_back_kernel(d_gate, d_up, w_gate, w_up, h, back, out):
    d_a = dot(d_gate[...], w_gate[...], (1, 1)) + dot(d_up[...], w_up[...], (1, 1))
    d_a, wide = d_a.astype(BF16).astype(F32), h[...].astype(F32)
    scale = lax.rsqrt(jnp.mean(wide**2, -1, keepdims=True) + 1e-6)
    inner = jnp.mean(d_a * wide, -1, keepdims=True)
    out[...] = back[...] + (scale * d_a - wide * (scale * scale * scale * inner)).astype(BF16)


def normed_back(d_gate, d_up, w_gate, w_up, h, back, layer, bt=256):
    tokens, d = h.shape
    ff = d_gate.shape[1]
    wide = pl.BlockSpec((bt, ff), lambda i: (i, 0))
    weight = pl.BlockSpec((None, d, ff), lambda i: (layer, 0, 0), pipeline_mode=pl.Buffered(1))
    narrow = pl.BlockSpec((bt, d), lambda i: (i, 0))
    return local_call(
        normed_back_kernel,
        "normed_back",
        4 * tokens * d * ff,
        4 * d * ff + 4 * tokens * ff,
        out_shape=jax.ShapeDtypeStruct((tokens, d), BF16),
        grid=(tokens // bt,),
        in_specs=[wide, wide, weight, weight, narrow, narrow],
        out_specs=narrow,
    )(d_gate, d_up, w_gate, w_up, h, back)


def place_kernel(rows, *refs):
    blocks, out = refs[0], refs[-1]
    parts = out.shape[2] // 2 // LANES

    def one(chip, _):
        for core in range(2):
            for part in range(parts):
                at = (core * parts + part) * LANES
                out[0, pl.ds(chip * rows, rows), at : at + LANES] = blocks[chip * 2 + core, part * rows : (part + 1) * rows, :]
        return 0

    lax.fori_loop(0, out.shape[1] // rows, one, 0)


def place(gathered, which, layer, shape, so_far, steps=8):
    _, total, width = shape
    rows = total // 64
    chips = 64 // steps
    size = gathered.shape[1] // 3
    in_specs = [pl.BlockSpec((2 * chips, size, LANES), lambda p: (p, which, 0))]
    args = [gathered]
    if so_far is not None:
        in_specs.append(pl.BlockSpec(memory_space=pl.ANY))
        args.append(so_far)
    return local_call(
        functools.partial(place_kernel, rows),
        "place",
        100_000_000,
        4 * total * width,
        out_shape=jax.ShapeDtypeStruct(shape, BF16),
        grid=(steps,),
        in_specs=in_specs,
        out_specs=pl.BlockSpec((1, rows * chips, width), lambda p: (layer, p, 0)),
        input_output_aliases={} if so_far is None else {1: 0},
    )(*args)


def tied(*ts):
    return lax.optimization_barrier(ts)


def gather(blocks):
    return lax.all_gather(blocks, ALL, axis=0, tiled=False)


def swap(t):
    return lax.ppermute(t, "core", [(0, 1), (1, 0)])


def scale_of(h):
    wide = h.astype(F32)
    return lax.rsqrt(jnp.mean(wide**2, -1, keepdims=True) + 1e-6)


def adamw(w, m, v, g):
    m = 0.9 * m + 0.1 * g
    v = 0.95 * v + 0.05 * g * g
    step = m * lax.rsqrt(v + 1e-8) + 0.1 * w
    return (w - 0.02 * step).astype(BF16), m, v


def local_step(x, dy, wg, wu, wd, *moments):
    ms, vs = moments[:3], moments[3:]
    weights = (wg, wu, wd)
    core = lax.axis_index("core")
    chip = (lax.axis_index("x") * N + lax.axis_index("y")) * N + lax.axis_index("z")
    which = core.astype(jnp.int32)[None]
    layers = wg.shape[0]

    h, back = x[0], dy[0]
    kept = []
    last = layers - 1
    back_other = swap(back)
    for n in range(layers):
        a = (h.astype(F32) * scale_of(h)).astype(BF16)
        a_other = swap(a)
        gate, up, act = gated(a, wg, wu, n)
        if n > 0:
            act, back_other, kept[n - 1][2], kept[n - 1][6] = tied(act, back_other, kept[n - 1][2], kept[n - 1][6])
        kept.append([h, a, a_other, gate, up, act, swap(act)])
        if n < last:
            h = h + dot(act, wd[n]).astype(BF16)

    new = [[None] * layers for _ in range(9)]
    placed = [None] * 3
    gathered = [None] * layers
    cut = lambda gs: [g.reshape(N, N, N, -1, g.shape[1]) for g in gs]
    for n in reversed(range(layers)):
        h, a, a_other, gate, up, act, act_other = kept[n]
        if n == last:
            d_gate, d_up = gated_back(back, wd, gate, up, n)
            d_up_other, d_gate_other = swap(d_up), swap(d_gate)
            below = normed_back(d_gate, d_up, wg, wu, h, back, n)
            d_gate, d_up, below = tied(d_gate, d_up, below)
            below_other = swap(below)
            by_gate = pair_gradient(which, a, a_other, d_gate, d_gate_other, 512)
            by_up = pair_gradient(which, a, a_other, d_up, d_up_other, 512)
            by_down = pair_gradient(which, act, act_other, back, back_other, 896)
            _, _, _, gate0, up0, act0, act0_other = kept[0]
            work = LayerBelow(*back.shape, gate0.shape[1])
            *sums, by_down0, d_gate, d_up, _, _, d_gate_other, d_up_other = sum_over_chips(
                cut((by_gate, by_up, by_down)), work, (act0, act0_other, below, below_other, wd, gate0, up0)
            )
        else:
            by_gate = pair_gradient(which, a, a_other, d_gate, d_gate_other, 512, True)
            d_up, pending = tied(d_up, pending)
            gathered[n + 1] = gather(pending)
            by_up = pair_gradient(which, a, a_other, d_up, d_up_other, 512, True)
            sums = sum_over_chips(cut((by_gate, by_up, by_down0)))
            tied_all = tied(*sums, *ms, *vs)
            sums, ms, vs = tied_all[:3], tied_all[3:6], tied_all[6:]

        blocks = []
        for k, total in enumerate(sums):
            other = swap(total)
            rows, half = total.shape[0] // 2, total.shape[1]
            halves = jnp.where(core == 0, jnp.stack([total, other]), jnp.stack([other, total]))
            mine = lax.dynamic_slice_in_dim(halves, core * rows, rows, 1)
            g = jnp.concatenate([mine[0], mine[1]], 1).astype(F32)
            at = (chip * 2 + core) * rows
            w = lax.dynamic_slice(weights[k], (n, at, 0), (1, rows, 2 * half))[0].astype(F32)
            w, m, v = adamw(w, ms[k][n], vs[k][n], g)
            new[3 + k][n], new[6 + k][n] = m, v
            keep = jnp.where(core == 0, w[:, :half], w[:, half:])
            give = jnp.where(core == 0, w[:, half:], w[:, :half])
            take = swap(give)
            both = jnp.where(core == 0, jnp.concatenate([keep, take], 0), jnp.concatenate([take, keep], 0))
            blocks += [both[:, i : i + LANES] for i in range(0, half, LANES)]
        pending = jnp.concatenate(blocks, 0)
        if n == 0:
            pending, *gathered[1:] = tied(pending, *gathered[1:])
            gathered[0] = gather(pending)

    for n in reversed(range(layers)):
        for k in range(3):
            placed[k] = place(gathered[n], k, n, weights[k].shape, placed[k])
    return (*placed, *(jnp.stack(new[i]) for i in range(3, 9)))


def solution(mesh):
    torus = Mesh(np.asarray(mesh.devices).reshape(N, N, N, 2), ALL)
    moments = P(None, ALL, None)
    return jax.shard_map(
        local_step,
        mesh=torus,
        in_specs=(P(ALL), P(ALL), P(), P(), P(), *([moments] * 6)),
        out_specs=(P(), P(), P(), *([moments] * 6)),
        check_vma=False,
    )
```

```python
import functools

import jax
import jax.numpy as jnp
import numpy as np
from jax import lax
from jax.experimental import pallas as pl
from jax.experimental.pallas import tpu as pltpu
from jax.sharding import Mesh
from jax.sharding import PartitionSpec as P

MESH = pl.DeviceIdType.MESH
RING = ("x", "y", "z")
ALL = ("x", "y", "z", "core")
N = 4
F32, BF16 = jnp.float32, jnp.bfloat16
LANES = 256


ORDERS = ((0, 1, 2), (1, 2, 0), (2, 0, 1))


def add_blocks(lead, out, *terms):
    def one(i, _):
        at = (i,) if len(lead) == 1 else (i // N, i % N)
        total = terms[0].at[at][...].astype(F32) if lead else None
        for t in terms[1:]:
            total = total + t.at[at][...].astype(F32)
        out.at[at][...] = total.astype(out.dtype)
        return 0

    if lead:
        lax.fori_loop(0, int(np.prod(lead)), one, 0)
    else:
        total = terms[0][...].astype(F32)
        for t in terms[1:]:
            total = total + t[...].astype(F32)
        out[...] = total.astype(out.dtype)


def scatter_kernel(layer, work, *refs):
    ins, made = (work.inputs, work.outputs) if work else (0, 0)
    grads, weights, moments, given, refs = refs[:3], refs[3:6], refs[6:12], refs[12 : 12 + ins], refs[12 + ins :]
    new_moments, block, making, scratch = refs[:6], refs[6], refs[7 : 7 + made], refs[7 + made :]
    per = 17
    me = [lax.axis_index(a) for a in RING]
    right = [lax.rem(i + 1, N) for i in me]
    left = [lax.rem(i + N - 1, N) for i in me]
    across = [lax.rem(i + 2, N) for i in me]

    barrier = pltpu.get_barrier_semaphore()
    for axis in range(3):
        for to in (right[axis], left[axis]):
            pl.semaphore_signal(barrier, inc=1, device_id={RING[axis]: to}, device_id_type=MESH)
    core = lax.axis_index("core")
    pl.semaphore_signal(barrier, inc=1, device_id={"core": 1 - core}, device_id_type=MESH)

    colours, tails = [], []
    for m in range(3):
        own, rx1, rx2, relay2, sum2, rx3, relay3, sum3, *tail = scratch[m * per : (m + 1) * per]
        tails.append(tail)
        colours.append((own, (rx1, rx2, rx3), (None, relay2, relay3), (None, sum2, sum3)))
    local_sem, send_sem, recv_sem, tail_sem, pair_send, pair_recv, *work_sem = scratch[3 * per :]

    def source(m, phase, index, half):
        own, _, _, sums = colours[m]
        a, b, _ = ORDERS[m]
        if phase == 0:
            width = grads[m].shape[-1] // 2
            at = [slice(None)] * 3
            at[a] = index
            return grads[m].at[(*at, slice(None), pl.ds(half * width, width))]
        if phase == 1:
            first = [axis for axis in range(3) if axis != a][0] == b
            return own.at[2 + half, index] if first else own.at[2 + half, :, index]
        return sums[1].at[half, index]

    loads = []
    for m in range(3):
        a = ORDERS[m][0]
        for k, (index, half) in enumerate(((right[a], 1), (left[a], 0), (me[a], 0), (me[a], 1))):
            copy = pltpu.make_async_copy(source(m, 0, index, half), colours[m][0].at[k], local_sem.at[m, k])
            copy.start()
            loads.append(copy)

    chip = (me[0] * N + me[1]) * N + me[2]
    for m in range(3):
        w, mom, vel = tails[m][:3]
        rows = w.shape[0]
        reads = (weights[m].at[layer, pl.ds(pl.multiple_of(chip * rows, 8), rows)], moments[m].at[layer], moments[3 + m].at[layer])
        for k, (src, dst) in enumerate(zip(reads, (w, mom, vel))):
            copy = pltpu.make_async_copy(src, dst, tail_sem.at[m, k])
            copy.start()
            loads.append(copy)

    pl.semaphore_wait(barrier, 7)

    pending = []
    for phase in range(3):
        lead = ((N, N), (N,), ())[phase]

        def send(m, k, src, to):
            axis = ORDERS[m][phase]
            copy = pltpu.make_async_remote_copy(
                src_ref=src,
                dst_ref=colours[m][1][phase].at[k],
                send_sem=send_sem.at[m, phase, k],
                recv_sem=recv_sem.at[m, phase, k],
                device_id={RING[axis]: to},
                device_id_type=MESH,
            )
            copy.start()
            pending.append(copy)
            return copy

        flights = []
        for m in range(3):
            axis = ORDERS[m][phase]
            flights.append(
                [
                    send(m, 0, source(m, phase, across[axis], 1), right[axis]),
                    send(m, 1, source(m, phase, across[axis], 0), left[axis]),
                ]
            )
        for m in range(3):
            axis = ORDERS[m][phase]
            flights[m] += [
                send(m, 2, source(m, phase, right[axis], 0), right[axis]),
                send(m, 3, source(m, phase, left[axis], 1), left[axis]),
            ]
        if phase == 0:
            for copy in loads:
                copy.wait()
            if work:
                work.first(given, making)
        for k in range(2):
            for m in range(3):
                axis = ORDERS[m][phase]
                own, rx, relays, _ = colours[m]
                flights[m][k].wait_recv()
                to = (right, left)[k][axis]
                if phase == 0:
                    passed = own.at[k]
                    add_blocks(lead, passed, passed, rx[phase].at[k])
                else:
                    passed = relays[phase].at[k]
                    add_blocks(lead, passed, source(m, phase, to, 1 - k), rx[phase].at[k])
                flights[m].append(send(m, 4 + k, passed, to))
        if phase == 0 and work:
            handed = work.second(given, making, *work_sem)
        for half in range(2):
            for m in range(3):
                axis = ORDERS[m][phase]
                own, rx, _, sums = colours[m]
                direct, relayed = (2, 5) if half == 0 else (3, 4)
                flights[m][direct].wait_recv()
                flights[m][relayed].wait_recv()
                mine = own.at[2 + half] if phase == 0 else source(m, phase, me[axis], half)
                target = mine if phase == 0 else sums[phase].at[half]
                add_blocks(lead, target, mine, rx[phase].at[direct], rx[phase].at[relayed])
    def swapped(m, k, src, dst):
        copy = pltpu.make_async_remote_copy(
            src_ref=src,
            dst_ref=dst,
            send_sem=pair_send.at[m, k],
            recv_sem=pair_recv.at[m, k],
            device_id={"core": 1 - core},
            device_id_type=MESH,
        )
        copy.start()
        return copy

    first = core == 0
    swaps = []
    for m in range(3):
        w, _, _, held, other, *_ = tails[m]
        width = held.shape[1] // 2
        for half in range(2):
            held[:, half * width : (half + 1) * width] = colours[m][3][2][half]
        swaps.append(swapped(m, 0, held, other))
    later = []
    for m in range(3):
        w, mom, vel, held, other, full, give, take, both = tails[m]
        rows, width = held.shape
        h = rows // 2
        full[...] = w[...].astype(F32)
        w_rows = jnp.where(first, full[:h, :], full[h:, :])
        swaps[m].wait()
        a, b = held[...].astype(F32), other[...].astype(F32)
        full[:, :width] = jnp.where(first, a, b)
        full[:, width:] = jnp.where(first, b, a)
        g = jnp.where(first, full[:h, :], full[h:, :])
        w_new, m_new, v_new = adamw(w_rows, mom[...], vel[...], g)
        new_moments[m][...] = m_new
        new_moments[3 + m][...] = v_new
        w_new = w_new.astype(F32)
        give[...] = jnp.where(first, w_new[:, width:], w_new[:, :width]).astype(BF16)
        both[:h, :] = jnp.where(first, w_new[:, :width], w_new[:, width:])
        later.append(swapped(m, 1, give, take))
    for m in range(3):
        take, both = tails[m][-2:]
        rows, width = both.shape
        h = rows // 2
        later[m].wait()
        kept, taken = both[:h, :], take[...].astype(F32)
        both[:h, :] = jnp.where(first, kept, taken)
        both[h:, :] = jnp.where(first, taken, kept)
        base = m * block.shape[0] // 3
        for part in range(width // LANES):
            at = base + part * rows
            block[at : at + rows, :] = both[:, part * LANES : (part + 1) * LANES].astype(BF16)
    for copy in pending:
        copy.wait_send()
    if work:
        for copy in handed:
            copy.wait()


def summed_and_updated(layer, grads, weights, moments, work=None, given=()):
    scratch = []
    for g, mom in zip(grads, moments):
        rows, width = g.shape[-2:]
        half, h = width // 2, rows // 2
        for lead in ((4, N, N), (6, N, N), (6, N), (2, N), (2, N), (6,), (2,), (2,)):
            scratch.append(pltpu.VMEM((*lead, rows, half), BF16))
        scratch += [
            pltpu.VMEM((rows, 2 * width), BF16),
            pltpu.VMEM((h, 2 * width), F32),
            pltpu.VMEM((h, 2 * width), F32),
            pltpu.VMEM((rows, width), BF16),
            pltpu.VMEM((rows, width), BF16),
            pltpu.VMEM((rows, 2 * width), F32),
            pltpu.VMEM((h, width), BF16),
            pltpu.VMEM((h, width), BF16),
            pltpu.VMEM((rows, width), F32),
        ]
    for shape in ((3, 4), (3, 3, 6), (3, 3, 6), (3, 3), (3, 2), (3, 2)):
        scratch.append(pltpu.SemaphoreType.DMA(shape))
    anywhere, vmem = pl.BlockSpec(memory_space=pl.ANY), pl.BlockSpec(memory_space=pltpu.VMEM)
    blocks = 3 * grads[0].shape[-2] * grads[0].shape[-1] // LANES
    out_shape = [jax.ShapeDtypeStruct(t.shape[1:], F32) for t in moments] + [jax.ShapeDtypeStruct((blocks, LANES), BF16)]
    out_specs = [vmem] * 7
    if work:
        scratch += [pltpu.SemaphoreType.DMA((2,)), pltpu.SemaphoreType.DMA((2,))]
        out_shape += work.shapes
        out_specs += [anywhere] * work.outputs
    return pl.pallas_call(
        functools.partial(scatter_kernel, layer, work),
        name="summed_and_updated",
        out_shape=out_shape,
        in_specs=[anywhere] * (12 + len(given)),
        out_specs=out_specs,
        scratch_shapes=scratch,
        compiler_params=pltpu.CompilerParams(collective_id=1 if work else 0, has_side_effects=True, vmem_limit_bytes=62 * 2**20),
        cost_estimate=pl.CostEstimate(flops=40_000_000_000, bytes_accessed=60_000_000, transcendentals=0),
    )(*grads, *weights, *moments, *given)


class LayerBelow:
    inputs, outputs = 7, 7

    def __init__(self, tokens, d, ff):
        self.tokens, self.d, self.ff = tokens, d, ff
        half = jax.ShapeDtypeStruct((tokens, ff // 2), BF16)
        self.shapes = [jax.ShapeDtypeStruct((ff, d // 2), BF16)] + [half] * 6

    def first(self, given, making, bm=512):
        act, act_other, back, back_other = given[:4]
        tokens, half = self.tokens, self.d // 2
        core = lax.axis_index("core")

        def step(act, act_other, back, back_other, out):
            dims = (((0,), (0,)), ((), ()))
            total = lax.dot_general(act[...], back[...], dims, preferred_element_type=F32)
            total = total + lax.dot_general(act_other[...], back_other[...], dims, preferred_element_type=F32)
            out[...] = total.astype(out.dtype)

        left = pl.BlockSpec((tokens, bm), lambda i: (0, i))
        side = pl.BlockSpec((tokens, half), lambda i: (0, core))
        pltpu.emit_pipeline(
            step,
            grid=(self.ff // bm,),
            in_specs=[left, left, side, side],
            out_specs=[pl.BlockSpec((bm, half), lambda i: (i, 0))],
        )(act, act_other, back, back_other, making[0])

    def second(self, given, making, send_sem, recv_sem, bn=256):
        back, w_down, gate, up = given[2], given[4], given[5], given[6]
        mine, theirs, others = making[1:3], making[3:5], making[5:7]
        core = lax.axis_index("core")
        blocks = self.ff // 2 // bn
        copies = []
        for half, outs in ((1 - core, theirs), (core, mine)):
            first = half * blocks
            wide = pl.BlockSpec((self.tokens, bn), lambda j, first=first: (0, first + j))
            out = pl.BlockSpec((self.tokens, bn), lambda j: (0, j))
            pltpu.emit_pipeline(
                gated_back_kernel,
                grid=(blocks,),
                in_specs=[
                    pl.BlockSpec((self.tokens, self.d), lambda j: (0, 0)),
                    pl.BlockSpec((bn, self.d), lambda j, first=first: (first + j, 0)),
                    wide,
                    wide,
                ],
                out_specs=[out, out],
            )(back, w_down.at[0], gate, up, *outs)
            if outs is theirs:
                for k in range(2):
                    copy = pltpu.make_async_remote_copy(
                        src_ref=theirs[k],
                        dst_ref=others[k],
                        send_sem=send_sem.at[k],
                        recv_sem=recv_sem.at[k],
                        device_id={"core": 1 - core},
                        device_id_type=MESH,
                    )
                    copy.start()
                    copies.append(copy)
        return copies


def grad_kernel(core, a, a_other, d, d_other, out):
    left, side = jnp.concatenate([a[...], a_other[...]], 0), jnp.concatenate([d[...], d_other[...]], 0)
    out[...] = lax.dot_general(left, side, (((0,), (0,)), ((), ())), preferred_element_type=F32).astype(out.dtype)


def pair_gradient(core, a, a_other, d, d_other, bm, halved=False):
    tokens, m = a.shape
    n = d.shape[1] if halved else d.shape[1] // 2
    left = pl.BlockSpec((tokens, bm), lambda i, core: (0, i))
    side = pl.BlockSpec((tokens, n), lambda i, core: (0, 0 if halved else core[0]))
    return pl.pallas_call(
        grad_kernel,
        name="pair_gradient",
        out_shape=jax.ShapeDtypeStruct((m, n), BF16),
        grid_spec=pltpu.PrefetchScalarGridSpec(
            num_scalar_prefetch=1,
            grid=(m // bm,),
            in_specs=[left, left, side, side],
            out_specs=pl.BlockSpec((bm, n), lambda i, core: (i, 0)),
        ),
        compiler_params=pltpu.CompilerParams(vmem_limit_bytes=60 * 2**20),
        cost_estimate=pl.CostEstimate(flops=4 * tokens * m * n, bytes_accessed=4 * tokens * (m + n) + 2 * m * n, transcendentals=0),
    )(core, a, a_other, d, d_other)


def dot(a, b, over=(1, 0)):
    return lax.dot_general(a, b, (((over[0],), (over[1],)), ((), ())), preferred_element_type=F32)


def local_call(body, name, flops, moved, **kw):
    return pl.pallas_call(
        body,
        name=name,
        compiler_params=pltpu.CompilerParams(vmem_limit_bytes=60 * 2**20),
        cost_estimate=pl.CostEstimate(flops=flops, bytes_accessed=moved, transcendentals=0),
        **kw,
    )


def gated_kernel(a, w_gate, w_up, gate, up, act):
    g, u = dot(a[...], w_gate[...]), dot(a[...], w_up[...])
    gate[...] = g
    up[...] = u
    act[...] = (g * jax.nn.sigmoid(g) * u).astype(act.dtype)


def gated(a, w_gate, w_up, layer, bn=512):
    tokens, d = a.shape
    ff = w_gate.shape[2]
    weight = pl.BlockSpec((None, d, bn), lambda j: (layer, 0, j))
    out = pl.BlockSpec((tokens, bn), lambda j: (0, j))
    return local_call(
        gated_kernel,
        "gated",
        4 * tokens * d * ff,
        4 * d * ff + 10 * tokens * ff,
        out_shape=[jax.ShapeDtypeStruct((tokens, ff), t) for t in (F32, F32, BF16)],
        grid=(ff // bn,),
        in_specs=[pl.BlockSpec((tokens, d), lambda j: (0, 0)), weight, weight],
        out_specs=[out] * 3,
    )(a, w_gate, w_up)


def gated_back_kernel(back, w_down, gate, up, d_gate, d_up):
    d_act = dot(back[...], w_down[...], (1, 1)).astype(BF16).astype(F32)
    g, u = gate[...], up[...]
    s = jax.nn.sigmoid(g)
    d_up[...] = (d_act * (g * s)).astype(d_up.dtype)
    d_gate[...] = (d_act * u * (s * (1 + g * (1 - s)))).astype(d_gate.dtype)


def gated_back(back, w_down, gate, up, layer, bn=512):
    tokens, d = back.shape
    ff = gate.shape[1]
    wide = pl.BlockSpec((tokens, bn), lambda j: (0, j))
    return local_call(
        gated_back_kernel,
        "gated_back",
        2 * tokens * d * ff,
        2 * d * ff + 12 * tokens * ff,
        out_shape=[jax.ShapeDtypeStruct((tokens, ff), BF16)] * 2,
        grid=(ff // bn,),
        in_specs=[pl.BlockSpec((tokens, d), lambda j: (0, 0)), pl.BlockSpec((None, bn, d), lambda j: (layer, j, 0)), wide, wide],
        out_specs=[wide] * 2,
    )(back, w_down, gate, up)


def normed_back_kernel(d_gate, d_up, w_gate, w_up, h, back, out):
    d_a = dot(d_gate[...], w_gate[...], (1, 1)) + dot(d_up[...], w_up[...], (1, 1))
    d_a, wide = d_a.astype(BF16).astype(F32), h[...].astype(F32)
    scale = lax.rsqrt(jnp.mean(wide**2, -1, keepdims=True) + 1e-6)
    inner = jnp.mean(d_a * wide, -1, keepdims=True)
    out[...] = back[...] + (scale * d_a - wide * (scale * scale * scale * inner)).astype(BF16)


def normed_back(d_gate, d_up, w_gate, w_up, h, back, layer, bt=256):
    tokens, d = h.shape
    ff = d_gate.shape[1]
    wide = pl.BlockSpec((bt, ff), lambda i: (i, 0))
    weight = pl.BlockSpec((None, d, ff), lambda i: (layer, 0, 0), pipeline_mode=pl.Buffered(1))
    narrow = pl.BlockSpec((bt, d), lambda i: (i, 0))
    return local_call(
        normed_back_kernel,
        "normed_back",
        4 * tokens * d * ff,
        4 * d * ff + 4 * tokens * ff,
        out_shape=jax.ShapeDtypeStruct((tokens, d), BF16),
        grid=(tokens // bt,),
        in_specs=[wide, wide, weight, weight, narrow, narrow],
        out_specs=narrow,
    )(d_gate, d_up, w_gate, w_up, h, back)


def place_kernel(rows, *refs):
    blocks, out = refs[0], refs[-1]
    parts = out.shape[2] // 2 // LANES

    def one(chip, _):
        for core in range(2):
            for part in range(parts):
                at = (core * parts + part) * LANES
                out[0, pl.ds(chip * rows, rows), at : at + LANES] = blocks[chip * 2 + core, part * rows : (part + 1) * rows, :]
        return 0

    lax.fori_loop(0, out.shape[1] // rows, one, 0)


def place(gathered, which, layer, shape, so_far, steps=16):
    _, total, width = shape
    rows = total // 64
    chips = 64 // steps
    size = gathered.shape[1] // 3
    in_specs = [pl.BlockSpec((2 * chips, size, LANES), lambda p: (p, which, 0))]
    args = [gathered]
    if so_far is not None:
        in_specs.append(pl.BlockSpec(memory_space=pl.ANY))
        args.append(so_far)
    return local_call(
        functools.partial(place_kernel, rows),
        "place",
        100_000_000,
        4 * total * width,
        out_shape=jax.ShapeDtypeStruct(shape, BF16),
        grid=(steps,),
        in_specs=in_specs,
        out_specs=pl.BlockSpec((1, rows * chips, width), lambda p: (layer, p, 0)),
        input_output_aliases={} if so_far is None else {1: 0},
    )(*args)


def tied(*ts):
    return lax.optimization_barrier(ts)


def gather(blocks):
    return lax.all_gather(blocks, ALL, axis=0, tiled=False)


def swap(t):
    return lax.ppermute(t, "core", [(0, 1), (1, 0)])


def scale_of(h):
    wide = h.astype(F32)
    return lax.rsqrt(jnp.mean(wide**2, -1, keepdims=True) + 1e-6)


def adamw(w, m, v, g):
    m = 0.9 * m + 0.1 * g
    v = 0.95 * v + 0.05 * g * g
    step = m * lax.rsqrt(v + 1e-8) + 0.1 * w
    return (w - 0.02 * step).astype(BF16), m, v


def local_step(x, dy, wg, wu, wd, *moments):
    weights = (wg, wu, wd)
    core = lax.axis_index("core")
    which = core.astype(jnp.int32)[None]
    layers = wg.shape[0]

    h, back = x[0], dy[0]
    kept = []
    last = layers - 1
    back_other = swap(back)
    for n in range(layers):
        a = (h.astype(F32) * scale_of(h)).astype(BF16)
        a_other = swap(a)
        gate, up, act = gated(a, wg, wu, n)
        if n > 0:
            act, back_other, kept[n - 1][2], kept[n - 1][6] = tied(act, back_other, kept[n - 1][2], kept[n - 1][6])
        kept.append([h, a, a_other, gate, up, act, swap(act)])
        if n < last:
            h = h + dot(act, wd[n]).astype(BF16)

    new = [[None] * layers for _ in range(9)]
    placed = [None] * 3
    gathered = [None] * layers
    cut = lambda gs: [g.reshape(N, N, N, -1, g.shape[1]) for g in gs]
    for n in reversed(range(layers)):
        h, a, a_other, gate, up, act, act_other = kept[n]
        if n == last:
            d_gate, d_up = gated_back(back, wd, gate, up, n)
            d_up_other, d_gate_other = swap(d_up), swap(d_gate)
            below = normed_back(d_gate, d_up, wg, wu, h, back, n)
            d_gate, d_up, below = tied(d_gate, d_up, below)
            below_other = swap(below)
            by_gate = pair_gradient(which, a, a_other, d_gate, d_gate_other, 512)
            by_up = pair_gradient(which, a, a_other, d_up, d_up_other, 512)
            by_down = pair_gradient(which, act, act_other, back, back_other, 896)
            _, _, _, gate0, up0, act0, act0_other = kept[0]
            work = LayerBelow(*back.shape, gate0.shape[1])
            *made, pending, by_down0, d_gate, d_up, _, _, d_gate_other, d_up_other = summed_and_updated(
                n, cut((by_gate, by_up, by_down)), weights, moments, work, (act0, act0_other, below, below_other, wd, gate0, up0)
            )
        else:
            by_gate = pair_gradient(which, a, a_other, d_gate, d_gate_other, 512, True)
            d_up, pending = tied(d_up, pending)
            gathered[n + 1] = gather(pending)
            by_up = pair_gradient(which, a, a_other, d_up, d_up_other, 512, True)
            *made, pending = summed_and_updated(n, cut((by_gate, by_up, by_down0)), weights, moments)
            pending, *gathered[1:] = tied(pending, *gathered[1:])
            gathered[0] = gather(pending)
        for k in range(6):
            new[3 + k][n] = made[k]

    for n in reversed(range(layers)):
        for k in range(3):
            placed[k] = place(gathered[n], k, n, weights[k].shape, placed[k])
    return (*placed, *(jnp.stack(new[i]) for i in range(3, 9)))


def solution(mesh):
    torus = Mesh(np.asarray(mesh.devices).reshape(N, N, N, 2), ALL)
    moments = P(None, ALL, None)
    return jax.shard_map(
        local_step,
        mesh=torus,
        in_specs=(P(ALL), P(ALL), P(), P(), P(), *([moments] * 6)),
        out_specs=(P(), P(), P(), *([moments] * 6)),
        check_vma=False,
    )
```

```python
import functools

import jax
import jax.numpy as jnp
import numpy as np
from jax import lax
from jax.experimental import pallas as pl
from jax.experimental.pallas import tpu as pltpu
from jax.sharding import Mesh
from jax.sharding import PartitionSpec as P

MESH = pl.DeviceIdType.MESH
RING = ("x", "y", "z")
ALL = ("x", "y", "z", "core")
N = 4
F32, BF16 = jnp.float32, jnp.bfloat16
LANES = 256


ORDERS = ((0, 1, 2), (1, 2, 0), (2, 0, 1))


def add_blocks(lead, out, *terms):
    def one(i, _):
        at = (i,) if len(lead) == 1 else (i // N, i % N)
        total = terms[0].at[at][...].astype(F32) if lead else None
        for t in terms[1:]:
            total = total + t.at[at][...].astype(F32)
        out.at[at][...] = total.astype(out.dtype)
        return 0

    if lead:
        lax.fori_loop(0, int(np.prod(lead)), one, 0)
    else:
        total = terms[0][...].astype(F32)
        for t in terms[1:]:
            total = total + t[...].astype(F32)
        out[...] = total.astype(out.dtype)


def scatter_kernel(layer, work, *refs):
    ins, made = (work.inputs, work.outputs) if work else (0, 0)
    grads, weights, moments, given, refs = refs[:3], refs[3:6], refs[6:12], refs[12 : 12 + ins], refs[12 + ins :]
    new_moments, block, making, scratch = refs[:6], refs[6], refs[7 : 7 + made], refs[7 + made :]
    per = 17
    me = [lax.axis_index(a) for a in RING]
    right = [lax.rem(i + 1, N) for i in me]
    left = [lax.rem(i + N - 1, N) for i in me]
    across = [lax.rem(i + 2, N) for i in me]

    barrier = pltpu.get_barrier_semaphore()
    for axis in range(3):
        for to in (right[axis], left[axis]):
            pl.semaphore_signal(barrier, inc=1, device_id={RING[axis]: to}, device_id_type=MESH)
    core = lax.axis_index("core")
    pl.semaphore_signal(barrier, inc=1, device_id={"core": 1 - core}, device_id_type=MESH)

    colours, tails = [], []
    for m in range(3):
        own, rx1, rx2, relay2, sum2, rx3, relay3, sum3, *tail = scratch[m * per : (m + 1) * per]
        tails.append(tail)
        colours.append((own, (rx1, rx2, rx3), (None, relay2, relay3), (None, sum2, sum3)))
    local_sem, send_sem, recv_sem, tail_sem, pair_send, pair_recv, *work_sem = scratch[3 * per :]

    def source(m, phase, index, half):
        own, _, _, sums = colours[m]
        a, b, _ = ORDERS[m]
        if phase == 0:
            width = grads[m].shape[-1] // 2
            at = [slice(None)] * 3
            at[a] = index
            return grads[m].at[(*at, slice(None), pl.ds(half * width, width))]
        if phase == 1:
            first = [axis for axis in range(3) if axis != a][0] == b
            return own.at[2 + half, index] if first else own.at[2 + half, :, index]
        return sums[1].at[half, index]

    loads = []
    for m in range(3):
        a = ORDERS[m][0]
        for k, (index, half) in enumerate(((right[a], 1), (left[a], 0), (me[a], 0), (me[a], 1))):
            copy = pltpu.make_async_copy(source(m, 0, index, half), colours[m][0].at[k], local_sem.at[m, k])
            copy.start()
            loads.append(copy)

    chip = (me[0] * N + me[1]) * N + me[2]
    for m in range(3):
        w, mom, vel = tails[m][:3]
        rows = w.shape[0]
        reads = (weights[m].at[layer, pl.ds(pl.multiple_of(chip * rows, 8), rows)], moments[m].at[layer], moments[3 + m].at[layer])
        for k, (src, dst) in enumerate(zip(reads, (w, mom, vel))):
            copy = pltpu.make_async_copy(src, dst, tail_sem.at[m, k])
            copy.start()
            loads.append(copy)

    pl.semaphore_wait(barrier, 7)

    pending = []
    for phase in range(3):
        lead = ((N, N), (N,), ())[phase]

        def send(m, k, src, to):
            axis = ORDERS[m][phase]
            copy = pltpu.make_async_remote_copy(
                src_ref=src,
                dst_ref=colours[m][1][phase].at[k],
                send_sem=send_sem.at[m, phase, k],
                recv_sem=recv_sem.at[m, phase, k],
                device_id={RING[axis]: to},
                device_id_type=MESH,
            )
            copy.start()
            pending.append(copy)
            return copy

        flights = []
        for m in range(3):
            axis = ORDERS[m][phase]
            flights.append(
                [
                    send(m, 0, source(m, phase, across[axis], 1), right[axis]),
                    send(m, 1, source(m, phase, across[axis], 0), left[axis]),
                ]
            )
        for m in range(3):
            axis = ORDERS[m][phase]
            flights[m] += [
                send(m, 2, source(m, phase, right[axis], 0), right[axis]),
                send(m, 3, source(m, phase, left[axis], 1), left[axis]),
            ]
        if phase == 0:
            for copy in loads:
                copy.wait()
            if work:
                work.first(given, making)
        for k in range(2):
            for m in range(3):
                axis = ORDERS[m][phase]
                own, rx, relays, _ = colours[m]
                flights[m][k].wait_recv()
                to = (right, left)[k][axis]
                if phase == 0:
                    passed = own.at[k]
                    add_blocks(lead, passed, passed, rx[phase].at[k])
                else:
                    passed = relays[phase].at[k]
                    add_blocks(lead, passed, source(m, phase, to, 1 - k), rx[phase].at[k])
                flights[m].append(send(m, 4 + k, passed, to))
        if phase == 0 and work:
            handed = work.second(given, making, *work_sem)
        for half in range(2):
            for m in range(3):
                axis = ORDERS[m][phase]
                own, rx, _, sums = colours[m]
                direct, relayed = (2, 5) if half == 0 else (3, 4)
                flights[m][direct].wait_recv()
                flights[m][relayed].wait_recv()
                mine = own.at[2 + half] if phase == 0 else source(m, phase, me[axis], half)
                target = mine if phase == 0 else sums[phase].at[half]
                add_blocks(lead, target, mine, rx[phase].at[direct], rx[phase].at[relayed])
    def swapped(m, k, src, dst):
        copy = pltpu.make_async_remote_copy(
            src_ref=src,
            dst_ref=dst,
            send_sem=pair_send.at[m, k],
            recv_sem=pair_recv.at[m, k],
            device_id={"core": 1 - core},
            device_id_type=MESH,
        )
        copy.start()
        return copy

    first = core == 0
    swaps = []
    for m in range(3):
        w, _, _, held, other, *_ = tails[m]
        width = held.shape[1] // 2
        for half in range(2):
            held[:, half * width : (half + 1) * width] = colours[m][3][2][half]
        swaps.append(swapped(m, 0, held, other))
    later = []
    for m in range(3):
        w, mom, vel, held, other, full, give, take, both = tails[m]
        rows, width = held.shape
        h = rows // 2
        full[...] = w[...].astype(F32)
        w_rows = jnp.where(first, full[:h, :], full[h:, :])
        swaps[m].wait()
        a, b = held[...].astype(F32), other[...].astype(F32)
        full[:, :width] = jnp.where(first, a, b)
        full[:, width:] = jnp.where(first, b, a)
        g = jnp.where(first, full[:h, :], full[h:, :])
        w_new, m_new, v_new = adamw(w_rows, mom[...], vel[...], g)
        new_moments[m][...] = m_new
        new_moments[3 + m][...] = v_new
        w_new = w_new.astype(F32)
        give[...] = jnp.where(first, w_new[:, width:], w_new[:, :width]).astype(BF16)
        both[:h, :] = jnp.where(first, w_new[:, :width], w_new[:, width:])
        later.append(swapped(m, 1, give, take))
    for m in range(3):
        take, both = tails[m][-2:]
        rows, width = both.shape
        h = rows // 2
        later[m].wait()
        kept, taken = both[:h, :], take[...].astype(F32)
        both[:h, :] = jnp.where(first, kept, taken)
        both[h:, :] = jnp.where(first, taken, kept)
        base = m * block.shape[0] // 3
        for part in range(width // LANES):
            at = base + part * rows
            block[at : at + rows, :] = both[:, part * LANES : (part + 1) * LANES].astype(BF16)
    for copy in pending:
        copy.wait_send()
    if work:
        for copy in handed:
            copy.wait()


def summed_and_updated(layer, grads, weights, moments, work=None, given=()):
    scratch = []
    for g, mom in zip(grads, moments):
        rows, width = g.shape[-2:]
        half, h = width // 2, rows // 2
        for lead in ((4, N, N), (6, N, N), (6, N), (2, N), (2, N), (6,), (2,), (2,)):
            scratch.append(pltpu.VMEM((*lead, rows, half), BF16))
        scratch += [
            pltpu.VMEM((rows, 2 * width), BF16),
            pltpu.VMEM((h, 2 * width), F32),
            pltpu.VMEM((h, 2 * width), F32),
            pltpu.VMEM((rows, width), BF16),
            pltpu.VMEM((rows, width), BF16),
            pltpu.VMEM((rows, 2 * width), F32),
            pltpu.VMEM((h, width), BF16),
            pltpu.VMEM((h, width), BF16),
            pltpu.VMEM((rows, width), F32),
        ]
    for shape in ((3, 4), (3, 3, 6), (3, 3, 6), (3, 3), (3, 2), (3, 2)):
        scratch.append(pltpu.SemaphoreType.DMA(shape))
    anywhere, vmem = pl.BlockSpec(memory_space=pl.ANY), pl.BlockSpec(memory_space=pltpu.VMEM)
    blocks = 3 * grads[0].shape[-2] * grads[0].shape[-1] // LANES
    out_shape = [jax.ShapeDtypeStruct(t.shape[1:], F32) for t in moments] + [jax.ShapeDtypeStruct((blocks, LANES), BF16)]
    out_specs = [vmem] * 7
    if work:
        scratch += [pltpu.SemaphoreType.DMA((2,)), pltpu.SemaphoreType.DMA((2,))]
        out_shape += work.shapes
        out_specs += [anywhere] * work.outputs
    return pl.pallas_call(
        functools.partial(scatter_kernel, layer, work),
        name="summed_and_updated",
        out_shape=out_shape,
        in_specs=[anywhere] * (12 + len(given)),
        out_specs=out_specs,
        scratch_shapes=scratch,
        compiler_params=pltpu.CompilerParams(collective_id=1 if work else 0, has_side_effects=True, vmem_limit_bytes=62 * 2**20),
        cost_estimate=pl.CostEstimate(flops=40_000_000_000, bytes_accessed=60_000_000, transcendentals=0),
    )(*grads, *weights, *moments, *given)


class LayerBelow:
    inputs, outputs = 7, 7

    def __init__(self, tokens, d, ff):
        self.tokens, self.d, self.ff = tokens, d, ff
        half = jax.ShapeDtypeStruct((tokens, ff // 2), BF16)
        self.shapes = [jax.ShapeDtypeStruct((ff, d // 2), BF16)] + [half] * 6

    def first(self, given, making, bm=512):
        act, act_other, back, back_other = given[:4]
        tokens, half = self.tokens, self.d // 2
        core = lax.axis_index("core")

        def step(act, act_other, back, back_other, out):
            dims = (((0,), (0,)), ((), ()))
            total = lax.dot_general(act[...], back[...], dims, preferred_element_type=F32)
            total = total + lax.dot_general(act_other[...], back_other[...], dims, preferred_element_type=F32)
            out[...] = total.astype(out.dtype)

        left = pl.BlockSpec((tokens, bm), lambda i: (0, i))
        side = pl.BlockSpec((tokens, half), lambda i: (0, core))
        pltpu.emit_pipeline(
            step,
            grid=(self.ff // bm,),
            in_specs=[left, left, side, side],
            out_specs=[pl.BlockSpec((bm, half), lambda i: (i, 0))],
        )(act, act_other, back, back_other, making[0])

    def second(self, given, making, send_sem, recv_sem, bn=256):
        back, w_down, gate, up = given[2], given[4], given[5], given[6]
        mine, theirs, others = making[1:3], making[3:5], making[5:7]
        core = lax.axis_index("core")
        blocks = self.ff // 2 // bn
        copies = []
        for half, outs in ((1 - core, theirs), (core, mine)):
            first = half * blocks
            wide = pl.BlockSpec((self.tokens, bn), lambda j, first=first: (0, first + j))
            out = pl.BlockSpec((self.tokens, bn), lambda j: (0, j))
            pltpu.emit_pipeline(
                gated_back_kernel,
                grid=(blocks,),
                in_specs=[
                    pl.BlockSpec((self.tokens, self.d), lambda j: (0, 0)),
                    pl.BlockSpec((bn, self.d), lambda j, first=first: (first + j, 0)),
                    wide,
                    wide,
                ],
                out_specs=[out, out],
            )(back, w_down.at[0], gate, up, *outs)
            if outs is theirs:
                for k in range(2):
                    copy = pltpu.make_async_remote_copy(
                        src_ref=theirs[k],
                        dst_ref=others[k],
                        send_sem=send_sem.at[k],
                        recv_sem=recv_sem.at[k],
                        device_id={"core": 1 - core},
                        device_id_type=MESH,
                    )
                    copy.start()
                    copies.append(copy)
        return copies


def grad_kernel(core, a, a_other, d, d_other, out):
    left, side = jnp.concatenate([a[...], a_other[...]], 0), jnp.concatenate([d[...], d_other[...]], 0)
    out[...] = lax.dot_general(left, side, (((0,), (0,)), ((), ())), preferred_element_type=F32).astype(out.dtype)


def pair_gradient(core, a, a_other, d, d_other, bm, halved=False):
    tokens, m = a.shape
    n = d.shape[1] if halved else d.shape[1] // 2
    left = pl.BlockSpec((tokens, bm), lambda i, core: (0, i))
    side = pl.BlockSpec((tokens, n), lambda i, core: (0, 0 if halved else core[0]))
    return pl.pallas_call(
        grad_kernel,
        name="pair_gradient",
        out_shape=jax.ShapeDtypeStruct((m, n), BF16),
        grid_spec=pltpu.PrefetchScalarGridSpec(
            num_scalar_prefetch=1,
            grid=(m // bm,),
            in_specs=[left, left, side, side],
            out_specs=pl.BlockSpec((bm, n), lambda i, core: (i, 0)),
        ),
        compiler_params=pltpu.CompilerParams(vmem_limit_bytes=60 * 2**20),
        cost_estimate=pl.CostEstimate(flops=4 * tokens * m * n, bytes_accessed=4 * tokens * (m + n) + 2 * m * n, transcendentals=0),
    )(core, a, a_other, d, d_other)


def dot(a, b, over=(1, 0)):
    return lax.dot_general(a, b, (((over[0],), (over[1],)), ((), ())), preferred_element_type=F32)


def local_call(body, name, flops, moved, **kw):
    return pl.pallas_call(
        body,
        name=name,
        compiler_params=pltpu.CompilerParams(vmem_limit_bytes=60 * 2**20),
        cost_estimate=pl.CostEstimate(flops=flops, bytes_accessed=moved, transcendentals=0),
        **kw,
    )


def gated_kernel(a, w_gate, w_up, gate, up, act):
    g, u = dot(a[...], w_gate[...]), dot(a[...], w_up[...])
    gate[...] = g
    up[...] = u
    act[...] = (g * jax.nn.sigmoid(g) * u).astype(act.dtype)


def gated(a, w_gate, w_up, layer, bn=512):
    tokens, d = a.shape
    ff = w_gate.shape[2]
    weight = pl.BlockSpec((None, d, bn), lambda j: (layer, 0, j))
    out = pl.BlockSpec((tokens, bn), lambda j: (0, j))
    return local_call(
        gated_kernel,
        "gated",
        4 * tokens * d * ff,
        4 * d * ff + 10 * tokens * ff,
        out_shape=[jax.ShapeDtypeStruct((tokens, ff), t) for t in (F32, F32, BF16)],
        grid=(ff // bn,),
        in_specs=[pl.BlockSpec((tokens, d), lambda j: (0, 0)), weight, weight],
        out_specs=[out] * 3,
    )(a, w_gate, w_up)


def gated_back_kernel(back, w_down, gate, up, d_gate, d_up):
    d_act = dot(back[...], w_down[...], (1, 1)).astype(BF16).astype(F32)
    g, u = gate[...], up[...]
    s = jax.nn.sigmoid(g)
    d_up[...] = (d_act * (g * s)).astype(d_up.dtype)
    d_gate[...] = (d_act * u * (s * (1 + g * (1 - s)))).astype(d_gate.dtype)


def turned_kernel(a, back, w_gate, w_up, w_down, act, d_gate, d_up):
    g, u = dot(a[...], w_gate[...]), dot(a[...], w_up[...])
    d_act = dot(back[...], w_down[...], (1, 1)).astype(BF16).astype(F32)
    s = jax.nn.sigmoid(g)
    gs = g * s
    act[...] = (gs * u).astype(act.dtype)
    d_up[...] = (d_act * gs).astype(d_up.dtype)
    d_gate[...] = (d_act * u * (s * (1 + g * (1 - s)))).astype(d_gate.dtype)


def turned(a, back, w_gate, w_up, w_down, layer, bn=512):
    tokens, d = a.shape
    ff = w_gate.shape[2]
    rows = pl.BlockSpec((tokens, d), lambda j: (0, 0))
    weight = pl.BlockSpec((None, d, bn), lambda j: (layer, 0, j))
    out = pl.BlockSpec((tokens, bn), lambda j: (0, j))
    return local_call(
        turned_kernel,
        "turned",
        6 * tokens * d * ff,
        6 * d * ff + 6 * tokens * ff,
        out_shape=[jax.ShapeDtypeStruct((tokens, ff), BF16)] * 3,
        grid=(ff // bn,),
        in_specs=[rows, rows, weight, weight, pl.BlockSpec((None, bn, d), lambda j: (layer, j, 0))],
        out_specs=[out] * 3,
    )(a, back, w_gate, w_up, w_down)


def normed_back_kernel(d_gate, d_up, w_gate, w_up, h, back, out):
    d_a = dot(d_gate[...], w_gate[...], (1, 1)) + dot(d_up[...], w_up[...], (1, 1))
    d_a, wide = d_a.astype(BF16).astype(F32), h[...].astype(F32)
    scale = lax.rsqrt(jnp.mean(wide**2, -1, keepdims=True) + 1e-6)
    inner = jnp.mean(d_a * wide, -1, keepdims=True)
    out[...] = back[...] + (scale * d_a - wide * (scale * scale * scale * inner)).astype(BF16)


def normed_back(d_gate, d_up, w_gate, w_up, h, back, layer, bt=256):
    tokens, d = h.shape
    ff = d_gate.shape[1]
    wide = pl.BlockSpec((bt, ff), lambda i: (i, 0))
    weight = pl.BlockSpec((None, d, ff), lambda i: (layer, 0, 0), pipeline_mode=pl.Buffered(1))
    narrow = pl.BlockSpec((bt, d), lambda i: (i, 0))
    return local_call(
        normed_back_kernel,
        "normed_back",
        4 * tokens * d * ff,
        4 * d * ff + 4 * tokens * ff,
        out_shape=jax.ShapeDtypeStruct((tokens, d), BF16),
        grid=(tokens // bt,),
        in_specs=[wide, wide, weight, weight, narrow, narrow],
        out_specs=narrow,
    )(d_gate, d_up, w_gate, w_up, h, back)


def place_kernel(*refs):
    blocks, outs = refs[:3], refs[-3:]
    for block, out in zip(blocks, outs):
        rows = block.shape[1] * LANES * 2 // out.shape[2]
        parts = out.shape[2] // 2 // LANES

        def one(chip, _):
            for core in range(2):
                for part in range(parts):
                    at = (core * parts + part) * LANES
                    out[0, pl.ds(chip * rows, rows), at : at + LANES] = block[chip * 2 + core, part * rows : (part + 1) * rows, :]
            return 0

        lax.fori_loop(0, out.shape[1] // rows, one, 0)


def place(gathered, layer, shapes, so_far, steps=4):
    devices, rows, _ = gathered.shape
    in_specs = [pl.BlockSpec((devices // steps, rows // 3, LANES), lambda p, k=k: (p, k, 0)) for k in range(3)]
    args = [gathered] * 3
    if so_far is not None:
        in_specs += [pl.BlockSpec(memory_space=pl.ANY)] * 3
        args += so_far
    return local_call(
        place_kernel,
        "place",
        300_000_000,
        4 * gathered.size,
        out_shape=[jax.ShapeDtypeStruct(shape, BF16) for shape in shapes],
        grid=(steps,),
        in_specs=in_specs,
        out_specs=[pl.BlockSpec((1, shape[1] // steps, shape[2]), lambda p: (layer, p, 0)) for shape in shapes],
        input_output_aliases={} if so_far is None else {3: 0, 4: 1, 5: 2},
    )(*args)


def tied(*ts):
    return lax.optimization_barrier(ts)


def gather(blocks):
    return lax.all_gather(blocks, ALL, axis=0, tiled=False)


def swap(t):
    return lax.ppermute(t, "core", [(0, 1), (1, 0)])


def scale_of(h):
    wide = h.astype(F32)
    return lax.rsqrt(jnp.mean(wide**2, -1, keepdims=True) + 1e-6)


def adamw(w, m, v, g):
    m = 0.9 * m + 0.1 * g
    v = 0.95 * v + 0.05 * g * g
    step = m * lax.rsqrt(v + 1e-8) + 0.1 * w
    return (w - 0.02 * step).astype(BF16), m, v


def local_step(x, dy, wg, wu, wd, *moments):
    weights = (wg, wu, wd)
    core = lax.axis_index("core")
    which = core.astype(jnp.int32)[None]
    layers = wg.shape[0]

    h, back = x[0], dy[0]
    kept = []
    last = layers - 1
    back_other = swap(back)
    for n in range(layers):
        a = (h.astype(F32) * scale_of(h)).astype(BF16)
        a_other = swap(a)
        if n == last:
            break
        gate, up, act = gated(a, wg, wu, n)
        kept.append((a, a_other, gate, up, act, swap(act)))
        h = h + dot(act, wd[n]).astype(BF16)

    new = [[None] * layers for _ in range(9)]
    gathered = [None] * layers
    cut = lambda gs: [g.reshape(N, N, N, -1, g.shape[1]) for g in gs]
    for n in reversed(range(layers)):
        if n == last:
            act, d_gate, d_up = turned(a, back, wg, wu, wd, n)
            a0, a0_other, gate0, up0, act0, act0_other = kept[0]
            d_gate, d_up, act, a_other, back_other, a0_other, act0_other = tied(d_gate, d_up, act, a_other, back_other, a0_other, act0_other)
            d_gate_other, d_up_other, act_other = swap(d_gate), swap(d_up), swap(act)
            below = normed_back(d_gate, d_up, wg, wu, h, back, n)
            d_gate, d_up, below = tied(d_gate, d_up, below)
            below_other = swap(below)
            by_gate = pair_gradient(which, a, a_other, d_gate, d_gate_other, 512)
            by_up = pair_gradient(which, a, a_other, d_up, d_up_other, 512)
            by_down = pair_gradient(which, act, act_other, back, back_other, 896)
            work = LayerBelow(*back.shape, gate0.shape[1])
            *made, pending, by_down0, d_gate, d_up, _, _, d_gate_other, d_up_other = summed_and_updated(
                n, cut((by_gate, by_up, by_down)), weights, moments, work, (act0, act0_other, below, below_other, wd, gate0, up0)
            )
        else:
            by_gate = pair_gradient(which, a0, a0_other, d_gate, d_gate_other, 512, True)
            d_up, pending = tied(d_up, pending)
            gathered[n + 1] = gather(pending)
            by_up = pair_gradient(which, a0, a0_other, d_up, d_up_other, 512, True)
            *made, pending = summed_and_updated(n, cut((by_gate, by_up, by_down0)), weights, moments)
            pending, *gathered[1:] = tied(pending, *gathered[1:])
            gathered[0] = gather(pending)
        for k in range(6):
            new[3 + k][n] = made[k]

    placed = None
    for n in reversed(range(layers)):
        placed = place(gathered[n], n, [w.shape for w in weights], placed)
    return (*placed, *(jnp.stack(new[i]) for i in range(3, 9)))


def solution(mesh):
    torus = Mesh(np.asarray(mesh.devices).reshape(N, N, N, 2), ALL)
    moments = P(None, ALL, None)
    return jax.shard_map(
        local_step,
        mesh=torus,
        in_specs=(P(ALL), P(ALL), P(), P(), P(), *([moments] * 6)),
        out_specs=(P(), P(), P(), *([moments] * 6)),
        check_vma=False,
    )
```

```python
import functools

import jax
import jax.numpy as jnp
import numpy as np
from jax import lax
from jax.experimental import pallas as pl
from jax.experimental.pallas import tpu as pltpu
from jax.sharding import Mesh
from jax.sharding import PartitionSpec as P

MESH = pl.DeviceIdType.MESH
RING = ("x", "y", "z")
ALL = ("x", "y", "z", "core")
N = 4
F32, BF16 = jnp.float32, jnp.bfloat16
LANES = 256


ORDERS = ((0, 1, 2), (1, 2, 0), (2, 0, 1))


def add_blocks(lead, out, *terms):
    def one(i, _):
        at = (i,) if len(lead) == 1 else (i // N, i % N)
        total = terms[0].at[at][...].astype(F32) if lead else None
        for t in terms[1:]:
            total = total + t.at[at][...].astype(F32)
        out.at[at][...] = total.astype(out.dtype)
        return 0

    if lead:
        lax.fori_loop(0, int(np.prod(lead)), one, 0)
    else:
        total = terms[0][...].astype(F32)
        for t in terms[1:]:
            total = total + t[...].astype(F32)
        out[...] = total.astype(out.dtype)


def scatter_kernel(layer, work, *refs):
    ins, made = (work.inputs, work.outputs) if work else (0, 0)
    grads, weights, moments, given, refs = refs[:3], refs[3:6], refs[6:12], refs[12 : 12 + ins], refs[12 + ins :]
    new_moments, block, making, scratch = refs[:6], refs[6], refs[7 : 7 + made], refs[7 + made :]
    per = 17
    me = [lax.axis_index(a) for a in RING]
    right = [lax.rem(i + 1, N) for i in me]
    left = [lax.rem(i + N - 1, N) for i in me]
    across = [lax.rem(i + 2, N) for i in me]

    barrier = pltpu.get_barrier_semaphore()
    for axis in range(3):
        for to in (right[axis], left[axis]):
            pl.semaphore_signal(barrier, inc=1, device_id={RING[axis]: to}, device_id_type=MESH)
    core = lax.axis_index("core")
    pl.semaphore_signal(barrier, inc=1, device_id={"core": 1 - core}, device_id_type=MESH)

    colours, tails = [], []
    for m in range(3):
        own, rx1, rx2, relay2, sum2, rx3, relay3, sum3, *tail = scratch[m * per : (m + 1) * per]
        tails.append(tail)
        colours.append((own, (rx1, rx2, rx3), (None, relay2, relay3), (None, sum2, sum3)))
    local_sem, send_sem, recv_sem, tail_sem, pair_send, pair_recv, *work_sem = scratch[3 * per :]

    def source(m, phase, index, half):
        own, _, _, sums = colours[m]
        a, b, _ = ORDERS[m]
        if phase == 0:
            width = grads[m].shape[-1] // 2
            at = [slice(None)] * 3
            at[a] = index
            return grads[m].at[(*at, slice(None), pl.ds(half * width, width))]
        if phase == 1:
            first = [axis for axis in range(3) if axis != a][0] == b
            return own.at[2 + half, index] if first else own.at[2 + half, :, index]
        return sums[1].at[half, index]

    loads = []
    for m in range(3):
        a = ORDERS[m][0]
        for k, (index, half) in enumerate(((right[a], 1), (left[a], 0), (me[a], 0), (me[a], 1))):
            copy = pltpu.make_async_copy(source(m, 0, index, half), colours[m][0].at[k], local_sem.at[m, k])
            copy.start()
            loads.append(copy)

    chip = (me[0] * N + me[1]) * N + me[2]
    for m in range(3):
        w, mom, vel = tails[m][:3]
        rows = w.shape[0]
        reads = (weights[m].at[layer, pl.ds(pl.multiple_of(chip * rows, 8), rows)], moments[m].at[layer], moments[3 + m].at[layer])
        for k, (src, dst) in enumerate(zip(reads, (w, mom, vel))):
            copy = pltpu.make_async_copy(src, dst, tail_sem.at[m, k])
            copy.start()
            loads.append(copy)

    pl.semaphore_wait(barrier, 7)

    pending = []
    for phase in range(3):
        lead = ((N, N), (N,), ())[phase]

        def send(m, k, src, to):
            axis = ORDERS[m][phase]
            copy = pltpu.make_async_remote_copy(
                src_ref=src,
                dst_ref=colours[m][1][phase].at[k],
                send_sem=send_sem.at[m, phase, k],
                recv_sem=recv_sem.at[m, phase, k],
                device_id={RING[axis]: to},
                device_id_type=MESH,
            )
            copy.start()
            pending.append(copy)
            return copy

        flights = []
        for m in range(3):
            axis = ORDERS[m][phase]
            flights.append(
                [
                    send(m, 0, source(m, phase, across[axis], 1), right[axis]),
                    send(m, 1, source(m, phase, across[axis], 0), left[axis]),
                ]
            )
        for m in range(3):
            axis = ORDERS[m][phase]
            flights[m] += [
                send(m, 2, source(m, phase, right[axis], 0), right[axis]),
                send(m, 3, source(m, phase, left[axis], 1), left[axis]),
            ]
        if phase == 0:
            for copy in loads:
                copy.wait()
            if work:
                work.first(given, making)
        for k in range(2):
            for m in range(3):
                axis = ORDERS[m][phase]
                own, rx, relays, _ = colours[m]
                flights[m][k].wait_recv()
                to = (right, left)[k][axis]
                if phase == 0:
                    passed = own.at[k]
                    add_blocks(lead, passed, passed, rx[phase].at[k])
                else:
                    passed = relays[phase].at[k]
                    add_blocks(lead, passed, source(m, phase, to, 1 - k), rx[phase].at[k])
                flights[m].append(send(m, 4 + k, passed, to))
        if phase == 0 and work:
            handed = work.second(given, making, *work_sem)
        for half in range(2):
            for m in range(3):
                axis = ORDERS[m][phase]
                own, rx, _, sums = colours[m]
                direct, relayed = (2, 5) if half == 0 else (3, 4)
                flights[m][direct].wait_recv()
                flights[m][relayed].wait_recv()
                mine = own.at[2 + half] if phase == 0 else source(m, phase, me[axis], half)
                target = mine if phase == 0 else sums[phase].at[half]
                add_blocks(lead, target, mine, rx[phase].at[direct], rx[phase].at[relayed])
    def swapped(m, k, src, dst):
        copy = pltpu.make_async_remote_copy(
            src_ref=src,
            dst_ref=dst,
            send_sem=pair_send.at[m, k],
            recv_sem=pair_recv.at[m, k],
            device_id={"core": 1 - core},
            device_id_type=MESH,
        )
        copy.start()
        return copy

    first = core == 0
    swaps = []
    for m in range(3):
        w, _, _, held, other, *_ = tails[m]
        width = held.shape[1] // 2
        for half in range(2):
            held[:, half * width : (half + 1) * width] = colours[m][3][2][half]
        swaps.append(swapped(m, 0, held, other))
    later = []
    for m in range(3):
        w, mom, vel, held, other, full, give, take, both = tails[m]
        rows, width = held.shape
        h = rows // 2
        full[...] = w[...].astype(F32)
        w_rows = jnp.where(first, full[:h, :], full[h:, :])
        swaps[m].wait()
        a, b = held[...].astype(F32), other[...].astype(F32)
        full[:, :width] = jnp.where(first, a, b)
        full[:, width:] = jnp.where(first, b, a)
        g = jnp.where(first, full[:h, :], full[h:, :])
        w_new, m_new, v_new = adamw(w_rows, mom[...], vel[...], g)
        new_moments[m][...] = m_new
        new_moments[3 + m][...] = v_new
        w_new = w_new.astype(F32)
        give[...] = jnp.where(first, w_new[:, width:], w_new[:, :width]).astype(BF16)
        both[:h, :] = jnp.where(first, w_new[:, :width], w_new[:, width:])
        later.append(swapped(m, 1, give, take))
    for m in range(3):
        take, both = tails[m][-2:]
        rows, width = both.shape
        h = rows // 2
        later[m].wait()
        kept, taken = both[:h, :], take[...].astype(F32)
        both[:h, :] = jnp.where(first, kept, taken)
        both[h:, :] = jnp.where(first, taken, kept)
        base = m * block.shape[0] // 3
        for part in range(width // LANES):
            at = base + part * rows
            block[at : at + rows, :] = both[:, part * LANES : (part + 1) * LANES].astype(BF16)
    for copy in pending:
        copy.wait_send()
    if work:
        for copy in handed:
            copy.wait()


def summed_and_updated(layer, grads, weights, moments, work=None, given=()):
    scratch = []
    for g, mom in zip(grads, moments):
        rows, width = g.shape[-2:]
        half, h = width // 2, rows // 2
        for lead in ((4, N, N), (6, N, N), (6, N), (2, N), (2, N), (6,), (2,), (2,)):
            scratch.append(pltpu.VMEM((*lead, rows, half), BF16))
        scratch += [
            pltpu.VMEM((rows, 2 * width), BF16),
            pltpu.VMEM((h, 2 * width), F32),
            pltpu.VMEM((h, 2 * width), F32),
            pltpu.VMEM((rows, width), BF16),
            pltpu.VMEM((rows, width), BF16),
            pltpu.VMEM((rows, 2 * width), F32),
            pltpu.VMEM((h, width), BF16),
            pltpu.VMEM((h, width), BF16),
            pltpu.VMEM((rows, width), F32),
        ]
    for shape in ((3, 4), (3, 3, 6), (3, 3, 6), (3, 3), (3, 2), (3, 2)):
        scratch.append(pltpu.SemaphoreType.DMA(shape))
    anywhere, vmem = pl.BlockSpec(memory_space=pl.ANY), pl.BlockSpec(memory_space=pltpu.VMEM)
    blocks = 3 * grads[0].shape[-2] * grads[0].shape[-1] // LANES
    out_shape = [jax.ShapeDtypeStruct(t.shape[1:], F32) for t in moments] + [jax.ShapeDtypeStruct((blocks, LANES), BF16)]
    out_specs = [vmem] * 7
    if work:
        scratch += [pltpu.SemaphoreType.DMA((2,)), pltpu.SemaphoreType.DMA((2,))]
        out_shape += work.shapes
        out_specs += [anywhere] * work.outputs
    return pl.pallas_call(
        functools.partial(scatter_kernel, layer, work),
        name="summed_and_updated",
        out_shape=out_shape,
        in_specs=[anywhere] * (12 + len(given)),
        out_specs=out_specs,
        scratch_shapes=scratch,
        compiler_params=pltpu.CompilerParams(collective_id=1 if work else 0, has_side_effects=True, vmem_limit_bytes=62 * 2**20),
        cost_estimate=pl.CostEstimate(flops=40_000_000_000, bytes_accessed=60_000_000, transcendentals=0),
    )(*grads, *weights, *moments, *given)


class LayerBelow:
    inputs, outputs = 7, 7

    def __init__(self, tokens, d, ff):
        self.tokens, self.d, self.ff = tokens, d, ff
        half = jax.ShapeDtypeStruct((tokens, ff // 2), BF16)
        self.shapes = [jax.ShapeDtypeStruct((ff, d // 2), BF16)] + [half] * 6

    def first(self, given, making, bm=512):
        act, act_other, back, back_other = given[:4]
        tokens, half = self.tokens, self.d // 2
        core = lax.axis_index("core")

        def step(act, act_other, back, back_other, out):
            dims = (((0,), (0,)), ((), ()))
            total = lax.dot_general(act[...], back[...], dims, preferred_element_type=F32)
            total = total + lax.dot_general(act_other[...], back_other[...], dims, preferred_element_type=F32)
            out[...] = total.astype(out.dtype)

        left = pl.BlockSpec((tokens, bm), lambda i: (0, i))
        side = pl.BlockSpec((tokens, half), lambda i: (0, core))
        pltpu.emit_pipeline(
            step,
            grid=(self.ff // bm,),
            in_specs=[left, left, side, side],
            out_specs=[pl.BlockSpec((bm, half), lambda i: (i, 0))],
        )(act, act_other, back, back_other, making[0])

    def second(self, given, making, send_sem, recv_sem, bn=256):
        back, w_down, gate, up = given[2], given[4], given[5], given[6]
        mine, theirs, others = making[1:3], making[3:5], making[5:7]
        core = lax.axis_index("core")
        blocks = self.ff // 2 // bn
        copies = []
        for half, outs in ((1 - core, theirs), (core, mine)):
            first = half * blocks
            wide = pl.BlockSpec((self.tokens, bn), lambda j, first=first: (0, first + j))
            out = pl.BlockSpec((self.tokens, bn), lambda j: (0, j))
            pltpu.emit_pipeline(
                gated_back_kernel,
                grid=(blocks,),
                in_specs=[
                    pl.BlockSpec((self.tokens, self.d), lambda j: (0, 0)),
                    pl.BlockSpec((bn, self.d), lambda j, first=first: (first + j, 0)),
                    wide,
                    wide,
                ],
                out_specs=[out, out],
            )(back, w_down.at[0], gate, up, *outs)
            if outs is theirs:
                for k in range(2):
                    copy = pltpu.make_async_remote_copy(
                        src_ref=theirs[k],
                        dst_ref=others[k],
                        send_sem=send_sem.at[k],
                        recv_sem=recv_sem.at[k],
                        device_id={"core": 1 - core},
                        device_id_type=MESH,
                    )
                    copy.start()
                    copies.append(copy)
        return copies


def grad_kernel(core, a, a_other, d, d_other, out):
    left, side = jnp.concatenate([a[...], a_other[...]], 0), jnp.concatenate([d[...], d_other[...]], 0)
    out[...] = lax.dot_general(left, side, (((0,), (0,)), ((), ())), preferred_element_type=F32).astype(out.dtype)


def pair_gradient(core, a, a_other, d, d_other, bm, halved=False):
    tokens, m = a.shape
    n = d.shape[1] if halved else d.shape[1] // 2
    left = pl.BlockSpec((tokens, bm), lambda i, core: (0, i))
    side = pl.BlockSpec((tokens, n), lambda i, core: (0, 0 if halved else core[0]))
    return pl.pallas_call(
        grad_kernel,
        name="pair_gradient",
        out_shape=jax.ShapeDtypeStruct((m, n), BF16),
        grid_spec=pltpu.PrefetchScalarGridSpec(
            num_scalar_prefetch=1,
            grid=(m // bm,),
            in_specs=[left, left, side, side],
            out_specs=pl.BlockSpec((bm, n), lambda i, core: (i, 0)),
        ),
        compiler_params=pltpu.CompilerParams(vmem_limit_bytes=60 * 2**20),
        cost_estimate=pl.CostEstimate(flops=4 * tokens * m * n, bytes_accessed=4 * tokens * (m + n) + 2 * m * n, transcendentals=0),
    )(core, a, a_other, d, d_other)


def dot(a, b, over=(1, 0)):
    return lax.dot_general(a, b, (((over[0],), (over[1],)), ((), ())), preferred_element_type=F32)


def local_call(body, name, flops, moved, **kw):
    return pl.pallas_call(
        body,
        name=name,
        compiler_params=pltpu.CompilerParams(vmem_limit_bytes=60 * 2**20),
        cost_estimate=pl.CostEstimate(flops=flops, bytes_accessed=moved, transcendentals=0),
        **kw,
    )


def gated_kernel(a, w_gate, w_up, gate, up, act):
    g, u = dot(a[...], w_gate[...]), dot(a[...], w_up[...])
    gate[...] = g
    up[...] = u
    act[...] = (g * jax.nn.sigmoid(g) * u).astype(act.dtype)


def gated(a, w_gate, w_up, layer, bn=512):
    tokens, d = a.shape
    ff = w_gate.shape[2]
    weight = pl.BlockSpec((None, d, bn), lambda j: (layer, 0, j))
    out = pl.BlockSpec((tokens, bn), lambda j: (0, j))
    return local_call(
        gated_kernel,
        "gated",
        4 * tokens * d * ff,
        4 * d * ff + 10 * tokens * ff,
        out_shape=[jax.ShapeDtypeStruct((tokens, ff), t) for t in (F32, F32, BF16)],
        grid=(ff // bn,),
        in_specs=[pl.BlockSpec((tokens, d), lambda j: (0, 0)), weight, weight],
        out_specs=[out] * 3,
    )(a, w_gate, w_up)


def gated_back_kernel(back, w_down, gate, up, d_gate, d_up):
    d_act = dot(back[...], w_down[...], (1, 1)).astype(BF16).astype(F32)
    g, u = gate[...], up[...]
    s = jax.nn.sigmoid(g)
    d_up[...] = (d_act * (g * s)).astype(d_up.dtype)
    d_gate[...] = (d_act * u * (s * (1 + g * (1 - s)))).astype(d_gate.dtype)


def turned_kernel(a, back, w_gate, w_up, w_down, act, d_gate, d_up):
    g, u = dot(a[...], w_gate[...]), dot(a[...], w_up[...])
    d_act = dot(back[...], w_down[...], (1, 1)).astype(BF16).astype(F32)
    s = jax.nn.sigmoid(g)
    gs = g * s
    act[...] = (gs * u).astype(act.dtype)
    d_up[...] = (d_act * gs).astype(d_up.dtype)
    d_gate[...] = (d_act * u * (s * (1 + g * (1 - s)))).astype(d_gate.dtype)


def turned(a, back, w_gate, w_up, w_down, layer, bn=512):
    tokens, d = a.shape
    ff = w_gate.shape[2]
    rows = pl.BlockSpec((tokens, d), lambda j: (0, 0))
    weight = pl.BlockSpec((None, d, bn), lambda j: (layer, 0, j))
    out = pl.BlockSpec((tokens, bn), lambda j: (0, j))
    return local_call(
        turned_kernel,
        "turned",
        6 * tokens * d * ff,
        6 * d * ff + 6 * tokens * ff,
        out_shape=[jax.ShapeDtypeStruct((tokens, ff), BF16)] * 3,
        grid=(ff // bn,),
        in_specs=[rows, rows, weight, weight, pl.BlockSpec((None, bn, d), lambda j: (layer, j, 0))],
        out_specs=[out] * 3,
    )(a, back, w_gate, w_up, w_down)


def normed_back_kernel(d_gate, d_up, w_gate, w_up, h, back, out):
    d_a = dot(d_gate[...], w_gate[...], (1, 1)) + dot(d_up[...], w_up[...], (1, 1))
    d_a, wide = d_a.astype(BF16).astype(F32), h[...].astype(F32)
    scale = lax.rsqrt(jnp.mean(wide**2, -1, keepdims=True) + 1e-6)
    inner = jnp.mean(d_a * wide, -1, keepdims=True)
    out[...] = back[...] + (scale * d_a - wide * (scale * scale * scale * inner)).astype(BF16)


def normed_back(d_gate, d_up, w_gate, w_up, h, back, layer, bt=256):
    tokens, d = h.shape
    ff = d_gate.shape[1]
    wide = pl.BlockSpec((bt, ff), lambda i: (i, 0))
    weight = pl.BlockSpec((None, d, ff), lambda i: (layer, 0, 0), pipeline_mode=pl.Buffered(1))
    narrow = pl.BlockSpec((bt, d), lambda i: (i, 0))
    return local_call(
        normed_back_kernel,
        "normed_back",
        4 * tokens * d * ff,
        4 * d * ff + 4 * tokens * ff,
        out_shape=jax.ShapeDtypeStruct((tokens, d), BF16),
        grid=(tokens // bt,),
        in_specs=[wide, wide, weight, weight, narrow, narrow],
        out_specs=narrow,
    )(d_gate, d_up, w_gate, w_up, h, back)


def place_kernel(*refs):
    blocks, outs = refs[:3], refs[-3:]
    for block, out in zip(blocks, outs):
        rows = block.shape[1] * LANES * 2 // out.shape[2]
        parts = out.shape[2] // 2 // LANES

        def one(chip, _):
            for core in range(2):
                for part in range(parts):
                    at = (core * parts + part) * LANES
                    out[0, pl.ds(chip * rows, rows), at : at + LANES] = block[chip * 2 + core, part * rows : (part + 1) * rows, :]
            return 0

        lax.fori_loop(0, out.shape[1] // rows, one, 0)


def place(gathered, layer, shapes, so_far, steps=4):
    devices, rows, _ = gathered.shape
    in_specs = [pl.BlockSpec((devices // steps, rows // 3, LANES), lambda p, k=k: (p, k, 0)) for k in range(3)]
    args = [gathered] * 3
    if so_far is not None:
        in_specs += [pl.BlockSpec(memory_space=pl.ANY)] * 3
        args += so_far
    return local_call(
        place_kernel,
        "place",
        300_000_000,
        4 * gathered.size,
        out_shape=[jax.ShapeDtypeStruct(shape, BF16) for shape in shapes],
        grid=(steps,),
        in_specs=in_specs,
        out_specs=[pl.BlockSpec((1, shape[1] // steps, shape[2]), lambda p: (layer, p, 0)) for shape in shapes],
        input_output_aliases={} if so_far is None else {3: 0, 4: 1, 5: 2},
    )(*args)


def tied(*ts):
    return lax.optimization_barrier(ts)


def gather(blocks):
    return lax.all_gather(blocks, ALL, axis=0, tiled=False)


def swap(t):
    return lax.ppermute(t, "core", [(0, 1), (1, 0)])


def scale_of(h):
    wide = h.astype(F32)
    return lax.rsqrt(jnp.mean(wide**2, -1, keepdims=True) + 1e-6)


def adamw(w, m, v, g):
    m = 0.9 * m + 0.1 * g
    v = 0.95 * v + 0.05 * g * g
    step = m * lax.rsqrt(v + 1e-8) + 0.1 * w
    return (w - 0.02 * step).astype(BF16), m, v


def local_step(x, dy, wg, wu, wd, *moments):
    weights = (wg, wu, wd)
    core = lax.axis_index("core")
    which = core.astype(jnp.int32)[None]
    layers = wg.shape[0]

    h, back = x[0], dy[0]
    kept = []
    last = layers - 1
    back_other = swap(back)
    for n in range(layers):
        a = (h.astype(F32) * scale_of(h)).astype(BF16)
        a_other = swap(a)
        if n == last:
            break
        gate, up, act = gated(a, wg, wu, n)
        kept.append((a, a_other, gate, up, act, swap(act)))
        h = h + dot(act, wd[n]).astype(BF16)

    new = [[None] * layers for _ in range(9)]
    gathered = [None] * layers
    cut = lambda gs: [g.reshape(N, N, N, -1, g.shape[1]) for g in gs]
    for n in reversed(range(layers)):
        if n == last:
            act, d_gate, d_up = turned(a, back, wg, wu, wd, n)
            a0, a0_other, gate0, up0, act0, act0_other = kept[0]
            d_gate, d_up, act, a_other, back_other, a0_other, act0_other = tied(d_gate, d_up, act, a_other, back_other, a0_other, act0_other)
            d_gate_other, d_up_other = swap(d_gate), swap(d_up)
            below = normed_back(d_gate, d_up, wg, wu, h, back, n)
            d_gate, d_up, act, below, d_gate_other, d_up_other = tied(d_gate, d_up, act, below, d_gate_other, d_up_other)
            below_other, act_other = swap(below), swap(act)
            by_gate = pair_gradient(which, a, a_other, d_gate, d_gate_other, 512)
            by_up = pair_gradient(which, a, a_other, d_up, d_up_other, 512)
            by_down = pair_gradient(which, act, act_other, back, back_other, 896)
            work = LayerBelow(*back.shape, gate0.shape[1])
            *made, pending, by_down0, d_gate, d_up, _, _, d_gate_other, d_up_other = summed_and_updated(
                n, cut((by_gate, by_up, by_down)), weights, moments, work, (act0, act0_other, below, below_other, wd, gate0, up0)
            )
        else:
            by_gate = pair_gradient(which, a0, a0_other, d_gate, d_gate_other, 512, True)
            d_up, pending = tied(d_up, pending)
            gathered[n + 1] = gather(pending)
            by_up = pair_gradient(which, a0, a0_other, d_up, d_up_other, 512, True)
            *made, pending = summed_and_updated(n, cut((by_gate, by_up, by_down0)), weights, moments)
            pending, *gathered[1:] = tied(pending, *gathered[1:])
            gathered[0] = gather(pending)
        for k in range(6):
            new[3 + k][n] = made[k]

    placed = None
    for n in reversed(range(layers)):
        placed = place(gathered[n], n, [w.shape for w in weights], placed)
    return (*placed, *(jnp.stack(new[i]) for i in range(3, 9)))


def solution(mesh):
    torus = Mesh(np.asarray(mesh.devices).reshape(N, N, N, 2), ALL)
    moments = P(None, ALL, None)
    return jax.shard_map(
        local_step,
        mesh=torus,
        in_specs=(P(ALL), P(ALL), P(), P(), P(), *([moments] * 6)),
        out_specs=(P(), P(), P(), *([moments] * 6)),
        check_vma=False,
    )
```
